768 devices in a mesh: region: 16 (over y, core), sub: 48 (over x, z).
Axes of the slice: x: 4, y: 8, z: 12, core: 2. Of those that a mesh axis runs over, the one named last changes fastest.
Arguments:
- coords: float32 [3, 49152, 128], P(None, ('region', 'sub')), may hold values from -3 to 3
- smooth: float32 [49152, 128], P(('region', 'sub')), may hold values from 0.6 to 1.5
- masses: float32 [49152, 128], P(('region', 'sub')), may hold values from 0.01 to 0.1
- owners: int32 [49152], P(('region', 'sub')), may hold values from 0 to 15, as said below
- counts: int32 [49152], P(('region', 'sub')), may hold values from 32 to 128
- neighbours: int32 [49152, 4], P(('region', 'sub')), may hold values from 0 to 71, as said below
Outputs:
- density: float32 [49152, 128], P(('region', 'sub'))
- accel: float32 [3, 49152, 128], P(None, ('region', 'sub'))
The draws below stay inside these ranges and needn't reach their ends.
Inputs may be any that keep to these rules, and one draw needn't show every extreme that they name: `owners`: within the 64 tiles of each device's block, every value 0 to 16 - 1 appears exactly 4 times. `neighbours`: the first entry of the list of slot t is 4 + t (the tile itself); the entries of one list are distinct and lie within 4 of 4 + t.
All inputs are finite; a program needn't handle non-finite values.
Results may differ from the reference program's by a relative error of at most 0.0001.
Values sent between devices are 32-bit elements; how exact they have to be, the bound alone decides.
A program may use at most 64 MiB of HBM per device.

```python
import math
import jax
import jax.numpy as jnp
from jax import lax

TILE_ROWS = 128
TILE_DEV = 64
HALO_TILES = 4
NEIGHBOURS = 4
PER_DEST = 4
TILES = 49152
N_REGION = 16
N_SUB = 48


def draw_owners(key, part):
    blocks = TILES // TILE_DEV
    key_list = jax.random.split(jax.random.fold_in(key, 11), blocks)

    def shuffled(sub_key):
        return jax.random.permutation(sub_key, TILE_DEV)
    permuted = jax.vmap(shuffled)(key_list)
    return (permuted // PER_DEST).reshape(-1).astype(jnp.int32)


def draw_neighbours(key, part):
    key_list = jax.random.split(jax.random.fold_in(key, 23), TILES)
    offsets = jnp.concatenate([jnp.arange(HALO_TILES, dtype=jnp.int32) - HALO_TILES, jnp.arange(HALO_TILES, dtype=jnp.int32) + 1])

    def choose_some(sub_key):
        return jax.random.permutation(sub_key, offsets)[:NEIGHBOURS - 1]
    chosen = jax.vmap(choose_some)(key_list)
    slot_index = jnp.arange(TILES, dtype=jnp.int32) % TILE_DEV + HALO_TILES
    return jnp.concatenate([slot_index[:, None], slot_index[:, None] + chosen], axis=1).astype(jnp.int32)


def with_ends(entries, key, smallest, top_value):
    place = [jax.random.randint(jax.random.fold_in(key, axis), (), 0, length) for axis, length in enumerate(entries.shape)]
    widest = entries.shape.index(max(entries.shape))
    neighbour = place[:widest] + [(place[widest] + 1) % entries.shape[widest]] + place[widest + 1:]
    return entries.at[tuple(place)].set(smallest).at[tuple(neighbour)].set(top_value)


def level_of(key, dims, cuts, least, top_value):
    loudness, own = 1.0, jax.random.fold_in(key, 6)
    for position, shards_of in cuts:
        heights = jnp.exp(jax.random.uniform(jax.random.fold_in(own, position), (shards_of,), jnp.float32, least / len(cuts), top_value / len(cuts)))
        loudness = loudness * jnp.repeat(heights, dims[position] // shards_of).reshape([-1 if axis == position else 1 for axis in range(len(dims))])
    return loudness


def centred(own_key, dims, spread, most, shards=(), held_as=jnp.bfloat16):
    entries = spread * jax.random.normal(own_key, dims, jnp.float32)
    if shards:
        entries = entries * level_of(own_key, dims, shards, -0.22, 0.18)
    return jnp.clip(entries, -most, most).astype(held_as)


def setup_inputs(seed: int = 0) -> dict:
    keys = jax.random.split(jax.random.key(seed), 7)
    return {
        "coords": centred(keys[0], (3, TILES, TILE_ROWS), 0.5, 3.0, ((1, 768),), jnp.float32),
        "smooth": jnp.clip(jnp.exp(math.log(1.5) - 0.9162907 * jax.random.uniform(keys[1], (TILES, TILE_ROWS), jnp.float32) ** level_of(keys[1], (TILES, TILE_ROWS), ((0, 768),), -0.2, 0.2)), 0.6, 1.5),
        "masses": jnp.clip(jnp.exp(math.log(0.1) - 2.3025851 * jax.random.uniform(keys[2], (TILES, TILE_ROWS), jnp.float32) ** level_of(keys[2], (TILES, TILE_ROWS), ((0, 768),), -0.2, 0.2)), 0.01, 0.1),
        "owners": draw_owners(jax.random.fold_in(keys[6], 71), 0),
        "counts": with_ends(jax.random.randint(keys[4], (TILES,), TILE_ROWS // 4, TILE_ROWS + 1), jax.random.fold_in(keys[4], 1), TILE_ROWS // 4, TILE_ROWS).astype(jnp.int32),
        "neighbours": draw_neighbours(jax.random.fold_in(keys[6], 71), 0),
    }


kernel_scale = math.pi ** -1.5


def pair_weights(pos_own, inverse_sq, kernel_norm, pos_partner):
    offset_vec = pos_own[:, :, :, None] - pos_partner[:, :, None, :]
    distance_sq = jnp.sum(offset_vec * offset_vec, axis=0)
    return offset_vec, jnp.exp(-distance_sq * inverse_sq[:, :, None]) * kernel_norm[:, :, None]


def own_part(extended, tile_dev):
    own_tiles = extended[:, HALO_TILES:HALO_TILES + tile_dev]
    smooth_len = own_tiles[3]
    inverse_sq = 1.0 / (smooth_len * smooth_len)
    kernel_norm = kernel_scale * inverse_sq / smooth_len
    return own_tiles, inverse_sq, kernel_norm


def density_pass(extended, neighbours):
    own_tiles, inverse_sq, kernel_norm = own_part(extended, neighbours.shape[0])
    partners = jnp.take(extended, neighbours, axis=1)
    density = jnp.zeros(inverse_sq.shape, jnp.float32)
    for nb_slot in range(neighbours.shape[1]):
        partner = partners[:, :, nb_slot]
        unused, weight_pair = pair_weights(own_tiles[:3], inverse_sq, kernel_norm, partner[:3])
        density = density + jnp.sum(weight_pair * partner[4][:, None, :], axis=-1)
    return density


def force_pass(extended, pressure_ext, neighbours, pressure_own):
    own_tiles, inverse_sq, kernel_norm = own_part(extended, neighbours.shape[0])
    partners = jnp.take(extended, neighbours, axis=1)
    pressure_nb = jnp.take(pressure_ext, neighbours, axis=0)
    accel_sum = jnp.zeros((3,) + inverse_sq.shape, jnp.float32)
    for nb_slot in range(neighbours.shape[1]):
        partner = partners[:, :, nb_slot]
        offset_vec, weight_pair = pair_weights(own_tiles[:3], inverse_sq, kernel_norm, partner[:3])
        coefficient = weight_pair * partner[4][:, None, :] * (pressure_own[:, :, None] + pressure_nb[:, nb_slot][:, None, :])
        accel_sum = accel_sum + jnp.sum(offset_vec * coefficient[None], axis=-1)
    return 2.0 * inverse_sq[None] * accel_sum


def with_rims(values, sub_axis, tile_axis):
    tile_dev = values.shape[tile_axis]
    below = lax.slice_in_dim(jnp.roll(values, 1, axis=sub_axis), tile_dev - HALO_TILES, tile_dev, axis=tile_axis)
    above = lax.slice_in_dim(jnp.roll(values, -1, axis=sub_axis), 0, HALO_TILES, axis=tile_axis)
    return jnp.concatenate([below, values, above], axis=tile_axis)


def density_block(bundle):
    return density_pass(bundle[0], bundle[1])


def force_block(bundle):
    return force_pass(bundle[0], bundle[1], bundle[2], bundle[3])


def reference(coords, smooth, masses, owners, counts, neighbours):
    regions = N_REGION
    subgroups = N_SUB
    tile_dev = TILE_DEV
    per_dest = tile_dev // regions
    blocks = regions * subgroups
    fields = jnp.concatenate([coords, smooth[None], masses[None]], axis=0)
    fields = fields.reshape(5, regions, subgroups, tile_dev, TILE_ROWS)
    ordering = jnp.argsort(owners.reshape(regions, subgroups, tile_dev), axis=-1, stable=True)
    index_full = jnp.broadcast_to(ordering[None, :, :, :, None], fields.shape)
    sorted_tiles = jnp.take_along_axis(fields, index_full, axis=3)
    arrived = sorted_tiles.reshape(5, regions, subgroups, regions, per_dest, TILE_ROWS)
    arrived = jnp.transpose(arrived, (0, 3, 2, 1, 4, 5)).reshape(5, regions, subgroups, tile_dev, TILE_ROWS)
    slot_ids = jnp.arange(TILE_ROWS, dtype=jnp.int32)
    live_mask = (slot_ids[None, None, None, :] < counts.reshape(regions, subgroups, tile_dev)[..., None]).astype(jnp.float32)
    outgoing = jnp.concatenate([arrived[:4], (arrived[4] * live_mask)[None]], axis=0)
    extended = with_rims(outgoing, 2, 3)
    ext_blocks = jnp.moveaxis(extended.reshape(5, blocks, tile_dev + 2 * HALO_TILES, TILE_ROWS), 1, 0)
    neighbour_blocks = neighbours.reshape(blocks, tile_dev, NEIGHBOURS)
    raw_density = lax.map(density_block, (ext_blocks, neighbour_blocks))
    live_blocks = live_mask.reshape(blocks, tile_dev, TILE_ROWS)
    safe_density = jnp.where(live_blocks > 0, raw_density, 1.0)
    pressure_own = jnp.where(live_blocks > 0, safe_density ** (-1.0 / 3.0), 0.0)
    pressure_ext = with_rims(pressure_own.reshape(regions, subgroups, tile_dev, TILE_ROWS), 1, 2)
    pressure_ext = pressure_ext.reshape(blocks, tile_dev + 2 * HALO_TILES, TILE_ROWS)
    accel_blocks = lax.map(force_block, (ext_blocks, pressure_ext, neighbour_blocks, pressure_own))
    density = (raw_density * live_blocks).reshape(blocks * tile_dev, TILE_ROWS)
    accel = jnp.moveaxis(accel_blocks * live_blocks[:, None], 1, 0).reshape(3, blocks * tile_dev, TILE_ROWS)
    return density, accel
```

```python
import functools
import math

import jax
import jax.numpy as jnp
from jax import lax
from jax.experimental import pallas as pl
from jax.experimental.pallas import tpu as pltpu
from jax.sharding import PartitionSpec as P

HALO = 4
FIELDS = 5
LOG2E = math.log2(math.e)
NORM_LOG2 = -1.5 * math.log2(math.pi)
DEAD_LOG2 = -1000.0
MESH = pl.DeviceIdType.MESH
F32 = jnp.float32
BF16 = jnp.bfloat16


def split3(v):
    hi = v.astype(BF16).astype(F32)
    rest = v - hi
    mid = rest.astype(BF16).astype(F32)
    return hi, mid, rest - mid


def relayout_kernel(regions, subs, coords_ref, smooth_ref, masses_ref, owners_ref, meta_ref,
                    fields_ref, meta_out_ref, packed, landed, meta_land,
                    send_sem, recv_sem, rim_send, rim_recv, meta_send, meta_recv):
    tile_dev = smooth_ref.shape[0]
    group = tile_dev // regions
    rim = 2 * HALO // group
    r = lax.axis_index("region")
    s = lax.axis_index("sub")
    up = lax.rem(s + 1, subs)
    down = lax.rem(s + subs - 1, subs)

    barrier = pltpu.get_barrier_semaphore()
    for off in range(1, regions):
        pl.semaphore_signal(barrier, inc=1, device_id=(lax.rem(r + off, regions), s), device_id_type=MESH)
    for peer in (up, down):
        pl.semaphore_signal(barrier, inc=1, device_id=(r, peer), device_id_type=MESH)

    own = owners_ref[...]
    hot = (lax.broadcasted_iota(jnp.int32, (regions, tile_dev), 0) == own).astype(F32)
    before = (lax.broadcasted_iota(jnp.int32, (tile_dev, tile_dev), 0)
              < lax.broadcasted_iota(jnp.int32, (tile_dev, tile_dev), 1)).astype(F32)
    count = jnp.dot(hot.astype(BF16), before.astype(BF16), preferred_element_type=F32)
    rank = jnp.sum(hot * count, axis=0, keepdims=True).astype(jnp.int32)
    place = own * 8 + rank
    pick = (lax.broadcasted_iota(jnp.int32, (8 * regions, tile_dev), 0) == place).astype(F32)
    pick3 = jnp.concatenate([pick, pick, pick], axis=1).astype(BF16)
    for f in range(FIELDS):
        field = coords_ref[f] if f < 3 else (smooth_ref[...] if f == 3 else masses_ref[...])
        stack = jnp.concatenate(split3(field), axis=0).astype(BF16)
        got = jnp.dot(pick3, stack, preferred_element_type=F32)
        for d in range(regions):
            packed[d, pl.ds(f, group, stride=FIELDS), :] = got[8 * d : 8 * d + group]

    pl.semaphore_wait(barrier, regions - 1 + 2)

    def meta_copy(slot, peer):
        return pltpu.make_async_remote_copy(
            src_ref=meta_ref, dst_ref=meta_land.at[slot], send_sem=meta_send.at[slot],
            recv_sem=meta_recv.at[slot], device_id=(r, peer), device_id_type=MESH)

    metas = [meta_copy(0, up), meta_copy(1, down)]
    offsets = sorted(range(1, regions), key=lambda o: -min(o, regions - o))
    copies = []
    for off in offsets:
        dst = lax.rem(r + off, regions)
        copies.append(pltpu.make_async_remote_copy(
            src_ref=packed.at[dst], dst_ref=landed.at[rim + r], send_sem=send_sem.at[off],
            recv_sem=recv_sem.at[r], device_id=(dst, s), device_id_type=MESH))
    for copy in copies:
        copy.start()
    for copy in metas:
        copy.start()
    landed[rim + r] = packed[r]

    def arrived(src):
        @pl.when(src != r)
        def _():
            pltpu.make_async_remote_copy(
                src_ref=packed.at[src], dst_ref=landed.at[rim + src], send_sem=send_sem.at[0],
                recv_sem=recv_sem.at[src], device_id=(src, s), device_id_type=MESH).wait_recv()

    first, last = list(range(rim)), list(range(regions - rim, regions))
    for src in first + [g for g in last if g not in first]:
        arrived(src)
    rims = [
        pltpu.make_async_remote_copy(
            src_ref=landed.at[pl.ds(rim, rim)], dst_ref=landed.at[pl.ds(rim + regions, rim)],
            send_sem=rim_send.at[0], recv_sem=rim_recv.at[0], device_id=(r, down), device_id_type=MESH),
        pltpu.make_async_remote_copy(
            src_ref=landed.at[pl.ds(regions, rim)], dst_ref=landed.at[pl.ds(0, rim)],
            send_sem=rim_send.at[1], recv_sem=rim_recv.at[1], device_id=(r, up), device_id_type=MESH),
    ]
    for copy in rims:
        copy.start()
    for src in range(regions):
        if src not in first + last:
            arrived(src)

    def unpack(groups):
        for g in groups:
            for f in range(FIELDS):
                fields_ref[f, group * g : group * (g + 1), :] = landed[g, pl.ds(f, group, stride=FIELDS), :]

    unpack(range(rim, rim + regions))
    for copy in metas:
        copy.wait_recv()
    meta_out_ref[...] = meta_land[...]
    for copy in rims:
        copy.wait_recv()
    unpack(list(range(rim)) + list(range(rim + regions, 2 * rim + regions)))
    for copy in copies + metas + rims:
        copy.wait_send()


def relayout(coords, smooth, masses, owners, meta):
    regions, subs = lax.axis_size("region"), lax.axis_size("sub")
    tile_dev, rows = smooth.shape
    group = tile_dev // regions
    groups = regions + 2 * (2 * HALO // group)
    vmem = pl.BlockSpec(memory_space=pltpu.VMEM)
    return pl.pallas_call(
        functools.partial(relayout_kernel, regions, subs),
        out_shape=(jax.ShapeDtypeStruct((FIELDS, groups * group, rows), F32),
                   jax.ShapeDtypeStruct((2,) + meta.shape, jnp.int32)),
        in_specs=[vmem] * 5,
        out_specs=(vmem, vmem),
        scratch_shapes=[
            pltpu.VMEM((regions, group * FIELDS, rows), F32),
            pltpu.VMEM((groups, group * FIELDS, rows), F32),
            pltpu.VMEM((2,) + meta.shape, jnp.int32),
            pltpu.SemaphoreType.DMA((regions,)),
            pltpu.SemaphoreType.DMA((regions,)),
            pltpu.SemaphoreType.DMA((2,)),
            pltpu.SemaphoreType.DMA((2,)),
            pltpu.SemaphoreType.DMA((2,)),
            pltpu.SemaphoreType.DMA((2,)),
        ],
        compiler_params=pltpu.CompilerParams(collective_id=0, has_side_effects=True),
        name="relayout",
    )(coords, smooth, masses, owners, meta)


def pair_kernel(fields_ref, live_ref, lists_ref, density_ref, accel_ref,
                partner8, own8, partner_t, weight_hi, weight_lo, raw, force8, force_f, sums8):
    n_ext, rows = live_ref.shape
    n_mid = n_ext - 2 * HALO
    n_own = n_mid - 2 * HALO
    live = live_ref[...] > 0
    x, y, z, h, m = (fields_ref[f] for f in range(FIELDS))
    norm_sq = x * x + y * y + z * z
    zero = jnp.zeros_like(x)
    one = jnp.ones_like(x)
    mass_log2 = jnp.where(live, jnp.log2(m), DEAD_LOG2)
    scale = LOG2E / (h * h)
    own_const = NORM_LOG2 - 3.0 * jnp.log2(h) - scale * norm_sq
    for k, v in enumerate((x, y, z, norm_sq, one, mass_log2, zero, zero)):
        partner8[pl.ds(k, n_ext, stride=8), :] = v
    twice = 2.0 * scale
    for k, v in enumerate((twice * x, twice * y, twice * z, -scale, own_const, one, zero, zero)):
        own8[pl.ds(k, n_ext, stride=8), :] = v

    def partner_step(e, carry):
        hi, mid, lo = split3(partner8[pl.ds(pl.multiple_of(e * 8, 8), 8), :])
        stack = jnp.concatenate([hi, mid, hi, mid, lo, hi], axis=0)
        partner_t[e] = stack.T.astype(BF16)
        return carry

    lax.fori_loop(0, n_ext, partner_step, 0, unroll=4)

    def weights_of(t):
        hi, mid, lo = split3(own8[pl.ds(pl.multiple_of((t + HALO) * 8, 8), 8), :])
        own = jnp.concatenate([hi, hi, mid, mid, hi, lo], axis=0).astype(BF16)
        return [jnp.exp2(jnp.dot(partner_t[lists_ref[4 * t + nb]], own, preferred_element_type=F32))
                for nb in range(4)]

    def add_up(weights):
        return sum(jnp.sum(w.reshape(rows // 8, 8, rows), axis=0) for w in weights)

    def rim_step(i, carry):
        t = jnp.where(i < HALO, i, i + n_own)
        raw[pl.ds(t, 1), :] = jnp.sum(add_up(weights_of(t)), axis=0, keepdims=True)
        return carry

    lax.fori_loop(0, 2 * HALO, rim_step, 0)

    def own_step(i, carry):
        t = i + HALO
        weights = weights_of(t)
        raw[pl.ds(t, 1), :] = jnp.sum(add_up(weights), axis=0, keepdims=True)
        for nb, w in enumerate(weights):
            hi = w.astype(BF16)
            weight_hi[i, nb * rows : (nb + 1) * rows, :] = hi
            weight_lo[i, nb * rows : (nb + 1) * rows, :] = (w - hi.astype(F32)).astype(BF16)
        return carry

    lax.fori_loop(0, n_own, own_step, 0)

    live_mid = live_ref[HALO : HALO + n_mid, :] > 0
    total = jnp.where(live_mid, raw[...], 1.0)
    q = jnp.where(live_mid, jnp.exp2(jnp.log2(total) * (-1.0 / 3.0)), 0.0)
    xm, ym, zm = (fields_ref[f, HALO : HALO + n_mid, :] for f in range(3))
    for k, v in enumerate((jnp.ones_like(q), xm, ym, zm, q, q * xm, q * ym, q * zm)):
        force8[pl.ds(k, n_mid, stride=8), :] = v

    def force_features(e, carry):
        v = force8[pl.ds(pl.multiple_of(e * 8, 8), 8), :]
        hi = v.astype(BF16)
        force_f[e] = jnp.concatenate([hi.astype(F32), v - hi.astype(F32)], axis=0).astype(BF16)
        return carry

    lax.fori_loop(0, n_mid, force_features, 0, unroll=4)

    def force_step(i, carry):
        base = 4 * (i + HALO)
        feats = jnp.concatenate([force_f[lists_ref[base + nb] - HALO] for nb in range(4)], axis=1)
        got = (jnp.dot(feats, weight_hi[i], preferred_element_type=F32)
               + jnp.dot(feats, weight_lo[i], preferred_element_type=F32))
        sums8[pl.ds(pl.multiple_of(i * 8, 8), 8), :] = got[:8] + got[8:]
        return carry

    lax.fori_loop(0, n_own, force_step, 0, unroll=2)

    mine = slice(2 * HALO, 2 * HALO + n_own)
    live_own = live_ref[mine, :] > 0
    qo = q[HALO : HALO + n_own]
    ho = fields_ref[3, mine, :]
    density_ref[...] = jnp.where(live_own, raw[HALO : HALO + n_own, :], 0.0)
    plain, pressed = (sums8[pl.ds(k, n_own, stride=8), :] for k in (0, 4))
    both = qo * plain + pressed
    factor = jnp.where(live_own, 2.0 / (ho * ho), 0.0)
    for k in range(3):
        near, far = (sums8[pl.ds(j + k, n_own, stride=8), :] for j in (1, 5))
        accel_ref[k] = factor * (fields_ref[k, mine, :] * both - (qo * near + far))


def pairs(fields, live, lists):
    n_ext, rows = live.shape
    n_mid, n_own = n_ext - 2 * HALO, n_ext - 4 * HALO
    vmem = pl.BlockSpec(memory_space=pltpu.VMEM)
    return pl.pallas_call(
        pair_kernel,
        out_shape=(jax.ShapeDtypeStruct((n_own, rows), F32), jax.ShapeDtypeStruct((3, n_own, rows), F32)),
        in_specs=[vmem, vmem, pl.BlockSpec(memory_space=pltpu.SMEM)],
        out_specs=(vmem, vmem),
        scratch_shapes=[
            pltpu.VMEM((n_ext * 8, rows), F32),
            pltpu.VMEM((n_ext * 8, rows), F32),
            pltpu.VMEM((n_ext, rows, 48), BF16),
            pltpu.VMEM((n_own, 4 * rows, rows), BF16),
            pltpu.VMEM((n_own, 4 * rows, rows), BF16),
            pltpu.VMEM((n_mid, rows), F32),
            pltpu.VMEM((n_mid * 8, rows), F32),
            pltpu.VMEM((n_mid, 16, rows), BF16),
            pltpu.VMEM((n_own * 8, rows), F32),
        ],
        name="pairs",
    )(fields, live, lists)


def per_device(coords, smooth, masses, owners, counts, neighbours):
    tile_dev, rows = smooth.shape
    flat = jnp.concatenate([counts, neighbours.reshape(-1)])
    pad = -flat.shape[0] % 128
    meta = jnp.pad(flat, (0, pad)).reshape(-1, 128)
    fields, rims = relayout(coords, smooth, masses, owners.reshape(1, -1), meta)
    rims = rims.reshape(2, -1)
    rim_counts, rim_lists = rims[:, :tile_dev], rims[:, tile_dev : 5 * tile_dev].reshape(2, tile_dev, 4)
    all_counts = jnp.concatenate([rim_counts[0, -2 * HALO :], counts, rim_counts[1, : 2 * HALO]])
    live = (jnp.arange(rows, dtype=jnp.int32)[None, :] < all_counts[:, None]).astype(jnp.int32)
    lists = jnp.concatenate([
        rim_lists[0, -HALO:] + (HALO - tile_dev), neighbours + HALO, rim_lists[1, :HALO] + (HALO + tile_dev),
    ]).reshape(-1)
    return pairs(fields, live, lists)


def solution(mesh):
    rs = ("region", "sub")
    in_specs = (P(None, rs, None), P(rs, None), P(rs, None), P(rs), P(rs), P(rs, None))
    out_specs = (P(rs, None), P(None, rs, None))
    return jax.shard_map(per_device, mesh=mesh, in_specs=in_specs, out_specs=out_specs, check_vma=False)
```

```python
import functools
import math

import jax
import jax.numpy as jnp
from jax import lax
from jax.experimental import pallas as pl
from jax.experimental.pallas import tpu as pltpu
from jax.sharding import PartitionSpec as P

HALO = 4
RIM = 2 * HALO
FIELDS = 5
UNROLL = 8
LOG2E = math.log2(math.e)
NORM_LOG2 = -1.5 * math.log2(math.pi)
DEAD_LOG2 = -1000.0
MESH = pl.DeviceIdType.MESH
F32 = jnp.float32
BF16 = jnp.bfloat16


def split3(v):
    hi = v.astype(BF16).astype(F32)
    rest = v - hi
    mid = rest.astype(BF16).astype(F32)
    return hi, mid, rest - mid


def kernel(regions, subs, coords_hbm, smooth_hbm, masses_hbm, owners_hbm, counts_hbm, lists_hbm,
           density_ref, accel_ref,
           coords, smooth, masses, owners, counts, lists, rim_counts_v, rim_lists_v, rim_counts, rim_lists,
           packed, landed, fields, live, partner8, own8, partner_t, weight_hi, weight_lo, raw, force8, force_f, sums8,
           in_sem, send_sem, recv_sem, rim_send, rim_recv, meta_send, meta_recv, meta_sem):
    tile_dev, rows = smooth.shape
    group = tile_dev // regions
    rim = RIM // group
    r = lax.axis_index("region")
    s = lax.axis_index("sub")
    up = lax.rem(s + 1, subs)
    down = lax.rem(s + subs - 1, subs)

    barrier = pltpu.get_barrier_semaphore()
    for off in range(1, regions):
        pl.semaphore_signal(barrier, inc=1, device_id=(lax.rem(r + off, regions), s), device_id_type=MESH)
    for peer in (up, down):
        pl.semaphore_signal(barrier, inc=1, device_id=(r, peer), device_id_type=MESH)
    loads = [pltpu.make_async_copy(src, dst, in_sem.at[n]) for n, (src, dst) in enumerate((
        (owners_hbm, owners), (coords_hbm, coords), (smooth_hbm, smooth), (masses_hbm, masses),
        (counts_hbm, counts), (lists_hbm, lists)))]
    for load in loads:
        load.start()

    loads[0].wait()
    own = owners[...]
    hot = (lax.broadcasted_iota(jnp.int32, (regions, tile_dev), 0) == own).astype(F32)
    before = (lax.broadcasted_iota(jnp.int32, (tile_dev, tile_dev), 0)
              < lax.broadcasted_iota(jnp.int32, (tile_dev, tile_dev), 1)).astype(F32)
    count = jnp.dot(hot.astype(BF16), before.astype(BF16), preferred_element_type=F32)
    rank = jnp.sum(hot * count, axis=0, keepdims=True).astype(jnp.int32)
    place = own * 8 + rank
    pick = (lax.broadcasted_iota(jnp.int32, (8 * regions, tile_dev), 0) == place).astype(F32)
    pick3 = jnp.concatenate([pick, pick, pick], axis=1).astype(BF16)
    for load in loads[1:4]:
        load.wait()
    for f in range(FIELDS):
        field = coords[f] if f < 3 else (smooth[...] if f == 3 else masses[...])
        stack = jnp.concatenate(split3(field), axis=0).astype(BF16)
        got = jnp.dot(pick3, stack, preferred_element_type=F32)
        for d in range(regions):
            packed[d, pl.ds(f, group, stride=FIELDS), :] = got[8 * d : 8 * d + group]

    pl.semaphore_wait(barrier, regions - 1 + 2)

    offsets = sorted(range(1, regions), key=lambda o: -min(o, regions - o))
    copies = []
    for off in offsets:
        dst = lax.rem(r + off, regions)
        copies.append(pltpu.make_async_remote_copy(
            src_ref=packed.at[dst], dst_ref=landed.at[rim + r], send_sem=send_sem.at[off],
            recv_sem=recv_sem.at[r], device_id=(dst, s), device_id_type=MESH))
    metas = [
        pltpu.make_async_remote_copy(
            src_ref=src, dst_ref=dst.at[slot], send_sem=meta_send.at[2 * n + slot],
            recv_sem=meta_recv.at[2 * n + slot], device_id=(r, peer), device_id_type=MESH)
        for slot, peer in enumerate((up, down))
        for n, (src, dst) in enumerate(((counts_hbm, rim_counts_v), (lists_hbm, rim_lists_v)))]
    for copy in copies + metas:
        copy.start()
    landed[rim + r] = packed[r]

    def arrived(src):
        @pl.when(src != r)
        def _():
            pltpu.make_async_remote_copy(
                src_ref=packed.at[src], dst_ref=landed.at[rim + src], send_sem=send_sem.at[0],
                recv_sem=recv_sem.at[src], device_id=(src, s), device_id_type=MESH).wait_recv()

    first = list(range(rim))
    first += [g for g in range(regions - rim, regions) if g not in first]
    for src in first:
        arrived(src)
    rims = [
        pltpu.make_async_remote_copy(
            src_ref=landed.at[pl.ds(rim, rim)], dst_ref=landed.at[pl.ds(rim + regions, rim)],
            send_sem=rim_send.at[0], recv_sem=rim_recv.at[0], device_id=(r, down), device_id_type=MESH),
        pltpu.make_async_remote_copy(
            src_ref=landed.at[pl.ds(regions, rim)], dst_ref=landed.at[pl.ds(0, rim)],
            send_sem=rim_send.at[1], recv_sem=rim_recv.at[1], device_id=(r, up), device_id_type=MESH),
    ]
    for copy in rims:
        copy.start()

    lane = lax.broadcasted_iota(jnp.int32, (1, rows), 1)
    for load in loads[4:]:
        load.wait()

    def live_step(t, carry):
        live[pl.ds(t + RIM, 1), :] = (lane < counts[0, t]).astype(F32)
        return carry

    lax.fori_loop(0, tile_dev, live_step, 0, unroll=UNROLL)
    for src in range(regions):
        if src not in first:
            arrived(src)

    def unpack(groups):
        for g in groups:
            for f in range(FIELDS):
                fields[f, group * g : group * (g + 1), :] = landed[g, pl.ds(f, group, stride=FIELDS), :]

    def pair_features(a, b):
        x, y, z, h, m = (fields[f, a:b, :] for f in range(FIELDS))
        norm_sq = x * x + y * y + z * z
        zero, one = jnp.zeros_like(x), jnp.ones_like(x)
        mass_log2 = jnp.where(live[a:b, :] > 0, jnp.log2(m), DEAD_LOG2)
        scale = LOG2E / (h * h)
        own_const = NORM_LOG2 - 3.0 * jnp.log2(h) - scale * norm_sq
        twice = 2.0 * scale
        for k, v in enumerate((x, y, z, norm_sq, one, mass_log2, zero, zero)):
            partner8[pl.ds(8 * a + k, b - a, stride=8), :] = v
        for k, v in enumerate((twice * x, twice * y, twice * z, -scale, own_const, one, zero, zero)):
            own8[pl.ds(8 * a + k, b - a, stride=8), :] = v

        def partner_step(e, carry):
            hi, mid, lo = split3(partner8[pl.ds(pl.multiple_of(e * 8, 8), 8), :])
            partner_t[e] = jnp.concatenate([hi, mid, hi, mid, lo, hi], axis=0).T.astype(BF16)
            return carry

        lax.fori_loop(a, b, partner_step, 0, unroll=UNROLL)

    def density_of(e, partners, slot):
        hi, mid, lo = split3(own8[pl.ds(pl.multiple_of(e * 8, 8), 8), :])
        mine = jnp.concatenate([hi, hi, mid, mid, hi, lo], axis=0).astype(BF16)
        total = None
        for nb, partner in enumerate(partners):
            w = jnp.exp2(jnp.dot(partner_t[partner], mine, preferred_element_type=F32))
            part = jnp.sum(w.reshape(rows // 8, 8, rows), axis=0)
            total = part if total is None else total + part
            if slot is not None:
                high = w.astype(BF16)
                weight_hi[slot, nb * rows : (nb + 1) * rows, :] = high
                weight_lo[slot, nb * rows : (nb + 1) * rows, :] = (w - high.astype(F32)).astype(BF16)
        raw[pl.ds(e, 1), :] = jnp.sum(total, axis=0, keepdims=True)

    def own_partners(t):
        return [lists[nb, t] + HALO for nb in range(4)]

    def pressures(a, b):
        alive = live[a:b, :] > 0
        total = jnp.where(alive, raw[a:b, :], 1.0)
        return jnp.where(alive, jnp.exp2(jnp.log2(total) * (-1.0 / 3.0)), 0.0)

    def force_features(a, b):
        q = pressures(a, b)
        x, y, z = (fields[f, a:b, :] for f in range(3))
        for k, v in enumerate((jnp.ones_like(q), x, y, z, q, q * x, q * y, q * z)):
            force8[pl.ds(8 * a + k, b - a, stride=8), :] = v

        def step(e, carry):
            v = force8[pl.ds(pl.multiple_of(e * 8, 8), 8), :]
            hi = v.astype(BF16).astype(F32)
            force_f[e] = jnp.concatenate([hi, v - hi], axis=0).astype(BF16)
            return carry

        lax.fori_loop(a, b, step, 0, unroll=UNROLL)

    def force_of(t):
        feats = jnp.concatenate([force_f[p] for p in own_partners(t)], axis=1)
        got = (jnp.dot(feats, weight_hi[t], preferred_element_type=F32)
               + jnp.dot(feats, weight_lo[t], preferred_element_type=F32))
        sums8[pl.ds(pl.multiple_of(t * 8, 8), 8), :] = got[:8] + got[8:]

    def finish(a, b):
        alive = live[RIM + a : RIM + b, :] > 0
        q = pressures(RIM + a, RIM + b)
        h = fields[3, RIM + a : RIM + b, :]
        density_ref[a:b, :] = jnp.where(alive, raw[RIM + a : RIM + b, :], 0.0)
        plain, pressed = (sums8[pl.ds(8 * a + k, b - a, stride=8), :] for k in (0, 4))
        both = q * plain + pressed
        factor = jnp.where(alive, 2.0 / (h * h), 0.0)
        for k in range(3):
            near, far = (sums8[pl.ds(8 * a + j + k, b - a, stride=8), :] for j in (1, 5))
            accel_ref[k, a:b, :] = factor * (fields[k, RIM + a : RIM + b, :] * both - (q * near + far))

    def inner_density(t, carry):
        density_of(t + RIM, own_partners(t), t)
        return carry

    def inner_force(t, carry):
        force_of(t)
        return carry

    top = RIM + tile_dev
    unpack(range(rim, rim + regions))
    pair_features(RIM, top)
    lax.fori_loop(HALO, tile_dev - HALO, inner_density, 0, unroll=UNROLL)
    force_features(RIM, top)
    lax.fori_loop(RIM, tile_dev - RIM, inner_force, 0, unroll=UNROLL)
    finish(RIM, tile_dev - RIM)

    for copy in metas:
        copy.wait_recv()
    moves = [pltpu.make_async_copy(rim_counts_v, rim_counts, meta_sem.at[0]),
             pltpu.make_async_copy(rim_lists_v, rim_lists, meta_sem.at[1])]
    for move in moves:
        move.start()
    for move in moves:
        move.wait()
    for copy in rims:
        copy.wait_recv()
    for k in range(RIM):
        live[k : k + 1, :] = (lane < rim_counts[0, 0, tile_dev - RIM + k]).astype(F32)
        live[top + k : top + k + 1, :] = (lane < rim_counts[1, 0, k]).astype(F32)
    unpack(list(range(rim)) + list(range(rim + regions, 2 * rim + regions)))
    pair_features(0, RIM)
    pair_features(top, top + RIM)
    for k in range(HALO):
        below = [jnp.maximum(rim_lists[0, nb, tile_dev - HALO + k] + (HALO - tile_dev), 0) for nb in range(4)]
        density_of(HALO + k, below, None)
        density_of(RIM + k, own_partners(k), k)
        density_of(top - HALO + k, own_partners(tile_dev - HALO + k), tile_dev - HALO + k)
        above = [rim_lists[1, nb, k] + (HALO + tile_dev) for nb in range(4)]
        density_of(top + k, above, None)
    force_features(0, 2 * RIM)
    force_features(top - RIM, top + RIM)
    for k in range(RIM):
        force_of(k)
        force_of(tile_dev - RIM + k)
    finish(0, RIM)
    finish(tile_dev - RIM, tile_dev)
    for copy in copies + metas + rims:
        copy.wait_send()


def per_device(coords, smooth, masses, owners, counts, neighbours):
    regions, subs = lax.axis_size("region"), lax.axis_size("sub")
    tile_dev, rows = smooth.shape
    group = tile_dev // regions
    groups = regions + 2 * (RIM // group)
    ext = tile_dev + 2 * RIM
    owners, counts, lists = owners.reshape(1, -1), counts.reshape(1, -1), neighbours.T
    vmem = pl.BlockSpec(memory_space=pltpu.VMEM)
    dma = pltpu.SemaphoreType.DMA
    return pl.pallas_call(
        functools.partial(kernel, regions, subs),
        out_shape=(jax.ShapeDtypeStruct((tile_dev, rows), F32), jax.ShapeDtypeStruct((3, tile_dev, rows), F32)),
        in_specs=[pl.BlockSpec(memory_space=pl.ANY)] * 6,
        out_specs=(vmem, vmem),
        scratch_shapes=[
            pltpu.VMEM(coords.shape, F32), pltpu.VMEM(smooth.shape, F32), pltpu.VMEM(masses.shape, F32),
            pltpu.VMEM(owners.shape, jnp.int32),
            pltpu.SMEM(counts.shape, jnp.int32), pltpu.SMEM(lists.shape, jnp.int32),
            pltpu.VMEM((2,) + counts.shape, jnp.int32), pltpu.VMEM((2,) + lists.shape, jnp.int32),
            pltpu.SMEM((2,) + counts.shape, jnp.int32), pltpu.SMEM((2,) + lists.shape, jnp.int32),
            pltpu.VMEM((regions, group * FIELDS, rows), F32),
            pltpu.VMEM((groups, group * FIELDS, rows), F32),
            pltpu.VMEM((FIELDS, ext, rows), F32),
            pltpu.VMEM((ext, rows), F32),
            pltpu.VMEM((ext * 8, rows), F32),
            pltpu.VMEM((ext * 8, rows), F32),
            pltpu.VMEM((ext, rows, 48), BF16),
            pltpu.VMEM((tile_dev, 4 * rows, rows), BF16),
            pltpu.VMEM((tile_dev, 4 * rows, rows), BF16),
            pltpu.VMEM((ext, rows), F32),
            pltpu.VMEM((ext * 8, rows), F32),
            pltpu.VMEM((ext, 16, rows), BF16),
            pltpu.VMEM((tile_dev * 8, rows), F32),
            dma((6,)), dma((regions,)), dma((regions,)), dma((2,)), dma((2,)), dma((4,)), dma((4,)), dma((2,)),
        ],
        compiler_params=pltpu.CompilerParams(collective_id=0, has_side_effects=True),
        name="sph",
    )(coords, smooth, masses, owners, counts, lists)


def solution(mesh):
    rs = ("region", "sub")
    in_specs = (P(None, rs, None), P(rs, None), P(rs, None), P(rs), P(rs), P(rs, None))
    out_specs = (P(rs, None), P(None, rs, None))
    return jax.shard_map(per_device, mesh=mesh, in_specs=in_specs, out_specs=out_specs, check_vma=False)
```

```python
import functools
import math

import jax
import jax.numpy as jnp
from jax import lax
from jax.experimental import pallas as pl
from jax.experimental.pallas import tpu as pltpu
from jax.sharding import PartitionSpec as P

HALO = 4
RIM = 2 * HALO
FIELDS = 5
UNROLL = 8
SUB_RUN = 12
LOG2E = math.log2(math.e)
NORM_LOG2 = -1.5 * math.log2(math.pi)
DEAD_LOG2 = -1000.0
MESH = pl.DeviceIdType.MESH
F32 = jnp.float32
BF16 = jnp.bfloat16


def split3(v):
    hi = v.astype(BF16).astype(F32)
    rest = v - hi
    mid = rest.astype(BF16).astype(F32)
    return hi, mid, rest - mid


def kernel(regions, subs, coords_hbm, smooth_hbm, masses_hbm, owners_hbm, counts_hbm, lists_hbm,
           density_ref, accel_ref,
           coords, smooth, masses, owners, counts, lists, rim_counts_v, rim_lists_v, rim_counts, rim_lists,
           packed, landed, fields, live, partner8, own8, partner_t, weight_hi, weight_lo, raw, force8, force_f, sums8,
           in_sem, send_sem, recv_sem, rim_send, rim_recv, meta_send, meta_recv, meta_sem, ok, rim_ok):
    tile_dev, rows = smooth.shape
    group = tile_dev // regions
    rim = RIM // group
    r = lax.axis_index("region")
    s = lax.axis_index("sub")
    up = lax.rem(s + 1, subs)
    down = lax.rem(s + subs - 1, subs)

    run = lax.rem(s, SUB_RUN) if subs % SUB_RUN == 0 else s
    last_run = (SUB_RUN if subs % SUB_RUN == 0 else subs) - 1
    down_earlier = run > 0
    up_earlier = run == last_run

    def order(i):
        chips = regions // 2
        y = i // 2
        place = 2 * jnp.where(y < chips // 2, y, chips + chips // 2 - 1 - y) + lax.rem(i, 2)
        return jnp.where(s == 0, jnp.where(i == 0, regions - 1, place - 1), place)

    mine = order(r)
    peers = [lax.rem(r + off, regions) for off in sorted(range(1, regions), key=lambda o: -min(o, regions - o))]
    later = [order(p) > mine for p in peers]

    def when_each(conditions, action):
        for n, condition in enumerate(conditions):
            pl.when(condition)(functools.partial(action, n))

    barrier = pltpu.get_barrier_semaphore()

    def greet(n):
        pl.semaphore_signal(barrier, inc=1, device_id=(peers[n], s), device_id_type=MESH)

    when_each(later, greet)

    def greet_rim(n):
        pl.semaphore_signal(barrier, inc=1, device_id=(r, (up, down)[n]), device_id_type=MESH)

    when_each([jnp.logical_not(up_earlier), jnp.logical_not(down_earlier)], greet_rim)
    loads = [pltpu.make_async_copy(src, dst, in_sem.at[n]) for n, (src, dst) in enumerate((
        (owners_hbm, owners), (coords_hbm, coords), (smooth_hbm, smooth), (masses_hbm, masses),
        (counts_hbm, counts), (lists_hbm, lists)))]
    for load in loads:
        load.start()
    expected = mine + down_earlier.astype(jnp.int32) + up_earlier.astype(jnp.int32)

    @pl.when(expected > 0)
    def _():
        pl.semaphore_wait(barrier, expected)

    def answer(n):
        pl.semaphore_signal(ok, inc=1, device_id=(peers[n], s), device_id_type=MESH)

    earlier = [jnp.logical_not(c) for c in later]
    when_each(earlier, answer)

    def answer_rim(n):
        pl.semaphore_signal(rim_ok.at[1 - n], inc=1, device_id=(r, (up, down)[n]), device_id_type=MESH)

    when_each([up_earlier, down_earlier], answer_rim)

    loads[0].wait()
    own = owners[...]
    hot = (lax.broadcasted_iota(jnp.int32, (regions, tile_dev), 0) == own).astype(F32)
    before = (lax.broadcasted_iota(jnp.int32, (tile_dev, tile_dev), 0)
              < lax.broadcasted_iota(jnp.int32, (tile_dev, tile_dev), 1)).astype(F32)
    count = jnp.dot(hot.astype(BF16), before.astype(BF16), preferred_element_type=F32)
    rank = jnp.sum(hot * count, axis=0, keepdims=True).astype(jnp.int32)
    place = own * 8 + rank
    pick = (lax.broadcasted_iota(jnp.int32, (8 * regions, tile_dev), 0) == place).astype(F32)
    pick3 = jnp.concatenate([pick, pick, pick], axis=1).astype(BF16)
    for load in loads[1:4]:
        load.wait()
    for f in range(FIELDS):
        field = coords[f] if f < 3 else (smooth[...] if f == 3 else masses[...])
        stack = jnp.concatenate(split3(field), axis=0).astype(BF16)
        got = jnp.dot(pick3, stack, preferred_element_type=F32)
        for d in range(regions):
            packed[d, pl.ds(f, group, stride=FIELDS), :] = got[8 * d : 8 * d + group]

    copies = [pltpu.make_async_remote_copy(
        src_ref=packed.at[dst], dst_ref=landed.at[rim + r], send_sem=send_sem.at[n],
        recv_sem=recv_sem.at[r], device_id=(dst, s), device_id_type=MESH) for n, dst in enumerate(peers)]
    metas = [[
        pltpu.make_async_remote_copy(
            src_ref=src, dst_ref=dst.at[slot], send_sem=meta_send.at[2 * n + slot],
            recv_sem=meta_recv.at[2 * n + slot], device_id=(r, peer), device_id_type=MESH)
        for n, (src, dst) in enumerate(((counts_hbm, rim_counts_v), (lists_hbm, rim_lists_v)))]
        for slot, peer in enumerate((up, down))]
    rims = [
        pltpu.make_async_remote_copy(
            src_ref=landed.at[pl.ds(regions, rim)], dst_ref=landed.at[pl.ds(0, rim)],
            send_sem=rim_send.at[0], recv_sem=rim_recv.at[0], device_id=(r, up), device_id_type=MESH),
        pltpu.make_async_remote_copy(
            src_ref=landed.at[pl.ds(rim, rim)], dst_ref=landed.at[pl.ds(rim + regions, rim)],
            send_sem=rim_send.at[1], recv_sem=rim_recv.at[1], device_id=(r, down), device_id_type=MESH),
    ]

    def send_meta(slot):
        for copy in metas[slot]:
            copy.start()

    def send_rim(slot):
        rims[slot].start()

    def answered_rim(slot):
        pl.semaphore_wait(rim_ok.at[slot], 1)
        send_meta(slot)
        send_rim(slot)

    when_each(earlier, lambda n: copies[n].start())
    when_each([up_earlier, down_earlier], send_meta)
    landed[rim + r] = packed[r]

    def arrived(src):
        @pl.when(src != r)
        def _():
            pltpu.make_async_remote_copy(
                src_ref=packed.at[src], dst_ref=landed.at[rim + src], send_sem=send_sem.at[0],
                recv_sem=recv_sem.at[src], device_id=(src, s), device_id_type=MESH).wait_recv()

    @pl.when(mine < regions - 1)
    def _():
        pl.semaphore_wait(ok, regions - 1 - mine)

    when_each(later, lambda n: copies[n].start())
    first = list(range(rim))
    first += [g for g in range(regions - rim, regions) if g not in first]
    for src in first:
        arrived(src)
    when_each([up_earlier, down_earlier], send_rim)
    pl.when(jnp.logical_not(up_earlier))(functools.partial(answered_rim, 0))

    lane = lax.broadcasted_iota(jnp.int32, (1, rows), 1)
    for load in loads[4:]:
        load.wait()

    def live_step(t, carry):
        live[pl.ds(t + RIM, 1), :] = (lane < counts[0, t]).astype(F32)
        return carry

    lax.fori_loop(0, tile_dev, live_step, 0, unroll=UNROLL)
    for src in range(regions):
        if src not in first:
            arrived(src)

    def unpack(groups):
        for g in groups:
            for f in range(FIELDS):
                fields[f, group * g : group * (g + 1), :] = landed[g, pl.ds(f, group, stride=FIELDS), :]

    def pair_features(a, b):
        x, y, z, h, m = (fields[f, a:b, :] for f in range(FIELDS))
        norm_sq = x * x + y * y + z * z
        zero, one = jnp.zeros_like(x), jnp.ones_like(x)
        mass_log2 = jnp.where(live[a:b, :] > 0, jnp.log2(m), DEAD_LOG2)
        scale = LOG2E / (h * h)
        own_const = NORM_LOG2 - 3.0 * jnp.log2(h) - scale * norm_sq
        twice = 2.0 * scale
        for k, v in enumerate((x, y, z, norm_sq, one, mass_log2, zero, zero)):
            partner8[pl.ds(8 * a + k, b - a, stride=8), :] = v
        for k, v in enumerate((twice * x, twice * y, twice * z, -scale, own_const, one, zero, zero)):
            own8[pl.ds(8 * a + k, b - a, stride=8), :] = v

        def partner_step(e, carry):
            hi, mid, lo = split3(partner8[pl.ds(pl.multiple_of(e * 8, 8), 8), :])
            partner_t[e] = jnp.concatenate([hi, mid, hi, mid, lo, hi], axis=0).T.astype(BF16)
            return carry

        lax.fori_loop(a, b, partner_step, 0, unroll=UNROLL)

    def density_of(e, partners, slot):
        hi, mid, lo = split3(own8[pl.ds(pl.multiple_of(e * 8, 8), 8), :])
        mine = jnp.concatenate([hi, hi, mid, mid, hi, lo], axis=0).astype(BF16)
        total = None
        for nb, partner in enumerate(partners):
            w = jnp.exp2(jnp.dot(partner_t[partner], mine, preferred_element_type=F32))
            part = jnp.sum(w.reshape(rows // 8, 8, rows), axis=0)
            total = part if total is None else total + part
            if slot is not None:
                high = w.astype(BF16)
                weight_hi[slot, nb * rows : (nb + 1) * rows, :] = high
                weight_lo[slot, nb * rows : (nb + 1) * rows, :] = (w - high.astype(F32)).astype(BF16)
        raw[pl.ds(e, 1), :] = jnp.sum(total, axis=0, keepdims=True)

    def own_partners(t):
        return [lists[nb, t] + HALO for nb in range(4)]

    def pressures(a, b):
        alive = live[a:b, :] > 0
        total = jnp.where(alive, raw[a:b, :], 1.0)
        return jnp.where(alive, jnp.exp2(jnp.log2(total) * (-1.0 / 3.0)), 0.0)

    def force_features(a, b):
        q = pressures(a, b)
        x, y, z = (fields[f, a:b, :] for f in range(3))
        for k, v in enumerate((jnp.ones_like(q), x, y, z, q, q * x, q * y, q * z)):
            force8[pl.ds(8 * a + k, b - a, stride=8), :] = v

        def step(e, carry):
            v = force8[pl.ds(pl.multiple_of(e * 8, 8), 8), :]
            hi = v.astype(BF16).astype(F32)
            force_f[e] = jnp.concatenate([hi, v - hi], axis=0).astype(BF16)
            return carry

        lax.fori_loop(a, b, step, 0, unroll=UNROLL)

    def force_of(t):
        feats = jnp.concatenate([force_f[p] for p in own_partners(t)], axis=1)
        got = (jnp.dot(feats, weight_hi[t], preferred_element_type=F32)
               + jnp.dot(feats, weight_lo[t], preferred_element_type=F32))
        sums8[pl.ds(pl.multiple_of(t * 8, 8), 8), :] = got[:8] + got[8:]

    def finish(a, b):
        alive = live[RIM + a : RIM + b, :] > 0
        q = pressures(RIM + a, RIM + b)
        h = fields[3, RIM + a : RIM + b, :]
        density_ref[a:b, :] = jnp.where(alive, raw[RIM + a : RIM + b, :], 0.0)
        plain, pressed = (sums8[pl.ds(8 * a + k, b - a, stride=8), :] for k in (0, 4))
        both = q * plain + pressed
        factor = jnp.where(alive, 2.0 / (h * h), 0.0)
        for k in range(3):
            near, far = (sums8[pl.ds(8 * a + j + k, b - a, stride=8), :] for j in (1, 5))
            accel_ref[k, a:b, :] = factor * (fields[k, RIM + a : RIM + b, :] * both - (q * near + far))

    def inner_density(t, carry):
        density_of(t + RIM, own_partners(t), t)
        return carry

    def inner_force(t, carry):
        force_of(t)
        return carry

    top = RIM + tile_dev
    unpack(range(rim, rim + regions))
    pair_features(RIM, top)
    lax.fori_loop(HALO, tile_dev - HALO, inner_density, 0, unroll=UNROLL)
    force_features(RIM, top)
    lax.fori_loop(RIM, tile_dev - RIM, inner_force, 0, unroll=UNROLL)
    finish(RIM, tile_dev - RIM)

    pl.when(jnp.logical_not(down_earlier))(functools.partial(answered_rim, 1))

    for copy in metas[0] + metas[1]:
        copy.wait_recv()
    moves = [pltpu.make_async_copy(rim_counts_v, rim_counts, meta_sem.at[0]),
             pltpu.make_async_copy(rim_lists_v, rim_lists, meta_sem.at[1])]
    for move in moves:
        move.start()
    for move in moves:
        move.wait()
    for k in range(RIM):
        live[k : k + 1, :] = (lane < rim_counts[0, 0, tile_dev - RIM + k]).astype(F32)
        live[top + k : top + k + 1, :] = (lane < rim_counts[1, 0, k]).astype(F32)

    rims[1].wait_recv()
    unpack(range(rim + regions, 2 * rim + regions))
    pair_features(top, top + RIM)
    for k in range(HALO):
        density_of(top - HALO + k, own_partners(tile_dev - HALO + k), tile_dev - HALO + k)
        above = [rim_lists[1, nb, k] + (HALO + tile_dev) for nb in range(4)]
        density_of(top + k, above, None)
    force_features(top - RIM, top + RIM)
    for k in range(RIM):
        force_of(tile_dev - RIM + k)
    finish(tile_dev - RIM, tile_dev)

    rims[0].wait_recv()
    unpack(range(rim))
    pair_features(0, RIM)
    for k in range(HALO):
        below = [jnp.maximum(rim_lists[0, nb, tile_dev - HALO + k] + (HALO - tile_dev), 0) for nb in range(4)]
        density_of(HALO + k, below, None)
        density_of(RIM + k, own_partners(k), k)
    force_features(0, 2 * RIM)
    for k in range(RIM):
        force_of(k)
    finish(0, RIM)
    for copy in copies + metas[0] + metas[1] + rims:
        copy.wait_send()


def per_device(coords, smooth, masses, owners, counts, neighbours):
    regions, subs = lax.axis_size("region"), lax.axis_size("sub")
    tile_dev, rows = smooth.shape
    group = tile_dev // regions
    groups = regions + 2 * (RIM // group)
    ext = tile_dev + 2 * RIM
    owners, counts, lists = owners.reshape(1, -1), counts.reshape(1, -1), neighbours.T
    vmem = pl.BlockSpec(memory_space=pltpu.VMEM)
    dma = pltpu.SemaphoreType.DMA
    return pl.pallas_call(
        functools.partial(kernel, regions, subs),
        out_shape=(pltpu.VMEM((tile_dev, rows), F32), pltpu.VMEM((3, tile_dev, rows), F32)),
        in_specs=[pl.BlockSpec(memory_space=pl.ANY)] * 6,
        out_specs=(vmem, vmem),
        scratch_shapes=[
            pltpu.VMEM(coords.shape, F32), pltpu.VMEM(smooth.shape, F32), pltpu.VMEM(masses.shape, F32),
            pltpu.VMEM(owners.shape, jnp.int32),
            pltpu.SMEM(counts.shape, jnp.int32), pltpu.SMEM(lists.shape, jnp.int32),
            pltpu.VMEM((2,) + counts.shape, jnp.int32), pltpu.VMEM((2,) + lists.shape, jnp.int32),
            pltpu.SMEM((2,) + counts.shape, jnp.int32), pltpu.SMEM((2,) + lists.shape, jnp.int32),
            pltpu.VMEM((regions, group * FIELDS, rows), F32),
            pltpu.VMEM((groups, group * FIELDS, rows), F32),
            pltpu.VMEM((FIELDS, ext, rows), F32),
            pltpu.VMEM((ext, rows), F32),
            pltpu.VMEM((ext * 8, rows), F32),
            pltpu.VMEM((ext * 8, rows), F32),
            pltpu.VMEM((ext, rows, 48), BF16),
            pltpu.VMEM((tile_dev, 4 * rows, rows), BF16),
            pltpu.VMEM((tile_dev, 4 * rows, rows), BF16),
            pltpu.VMEM((ext, rows), F32),
            pltpu.VMEM((ext * 8, rows), F32),
            pltpu.VMEM((ext, 16, rows), BF16),
            pltpu.VMEM((tile_dev * 8, rows), F32),
            dma((6,)), dma((regions,)), dma((regions,)), dma((2,)), dma((2,)), dma((4,)), dma((4,)), dma((2,)),
            pltpu.SemaphoreType.REGULAR, pltpu.SemaphoreType.REGULAR((2,)),
        ],
        compiler_params=pltpu.CompilerParams(collective_id=0, has_side_effects=True),
        name="sph",
    )(coords, smooth, masses, owners, counts, lists)


def solution(mesh):
    rs = ("region", "sub")
    in_specs = (P(None, rs, None), P(rs, None), P(rs, None), P(rs), P(rs), P(rs, None))
    out_specs = (P(rs, None), P(None, rs, None))
    return jax.shard_map(per_device, mesh=mesh, in_specs=in_specs, out_specs=out_specs, check_vma=False)
```

```python
import functools
import math

import jax
import jax.numpy as jnp
from jax import lax
from jax.experimental import pallas as pl
from jax.experimental.pallas import tpu as pltpu
from jax.sharding import PartitionSpec as P

HALO = 4
RIM = 2 * HALO
FIELDS = 5
UNROLL = 8
SUB_RUN = 12
LOG2E = math.log2(math.e)
NORM_LOG2 = -1.5 * math.log2(math.pi)
DEAD_LOG2 = -1000.0
MESH = pl.DeviceIdType.MESH
F32 = jnp.float32
BF16 = jnp.bfloat16


def largest(n, most=13):
    return max(k for k in range(1, most + 1) if n % k == 0)


def split3(v):
    hi = v.astype(BF16).astype(F32)
    rest = v - hi
    mid = rest.astype(BF16).astype(F32)
    return hi, mid, rest - mid


def kernel(regions, subs, coords_hbm, smooth_hbm, masses_hbm, owners_hbm, counts_hbm, lists_hbm,
           density_ref, accel_ref,
           coords, smooth, masses, owners, counts, lists, rim_counts_v, rim_lists_v, rim_counts, rim_lists,
           packed, landed, fields, live, partner8, own8, partner_t, weight_hi, weight_lo, raw, force8, force_f, sums8,
           in_sem, send_sem, recv_sem, rim_send, rim_recv, meta_send, meta_recv, meta_sem, ok, rim_ok):
    tile_dev, rows = smooth.shape
    group = tile_dev // regions
    rim = RIM // group
    r = lax.axis_index("region")
    s = lax.axis_index("sub")
    up = lax.rem(s + 1, subs)
    down = lax.rem(s + subs - 1, subs)

    run = lax.rem(s, SUB_RUN) if subs % SUB_RUN == 0 else s
    last_run = (SUB_RUN if subs % SUB_RUN == 0 else subs) - 1
    down_earlier = run > 0
    up_earlier = run == last_run

    def partner(k):
        chips = regions // 2

        def at(k):
            y = k // 2
            return 2 * (y if y < chips // 2 else chips + chips // 2 - 1 - y) + k % 2

        return jnp.where(s == 0, 0 if k == regions - 1 else at(k + 1), at(k))

    def order(i):
        chips = regions // 2
        y = i // 2
        place = 2 * jnp.where(y < chips // 2, y, chips + chips // 2 - 1 - y) + lax.rem(i, 2)
        return jnp.where(s == 0, jnp.where(i == 0, regions - 1, place - 1), place)

    mine = order(r)
    peers = [partner(k) for k in range(regions)]
    later = [mine < k for k in range(regions)]
    earlier = [mine > k for k in range(regions)]

    def when_each(conditions, action):
        for n, condition in enumerate(conditions):
            pl.when(condition)(functools.partial(action, n))

    barrier = pltpu.get_barrier_semaphore()

    def greet(n):
        pl.semaphore_signal(barrier, inc=1, device_id=(peers[n], s), device_id_type=MESH)

    when_each(later, greet)

    def greet_rim(n):
        pl.semaphore_signal(barrier, inc=1, device_id=(r, (up, down)[n]), device_id_type=MESH)

    when_each([jnp.logical_not(up_earlier), jnp.logical_not(down_earlier)], greet_rim)
    loads = [pltpu.make_async_copy(src, dst, in_sem.at[n]) for n, (src, dst) in enumerate((
        (owners_hbm, owners), (coords_hbm, coords), (smooth_hbm, smooth), (masses_hbm, masses),
        (counts_hbm, counts), (lists_hbm, lists)))]
    for load in loads:
        load.start()
    expected = mine + down_earlier.astype(jnp.int32) + up_earlier.astype(jnp.int32)

    @pl.when(expected > 0)
    def _():
        pl.semaphore_wait(barrier, expected)

    def answer(n):
        pl.semaphore_signal(ok.at[r], inc=1, device_id=(peers[n], s), device_id_type=MESH)

    when_each(earlier, answer)

    def answer_rim(n):
        pl.semaphore_signal(rim_ok.at[1 - n], inc=1, device_id=(r, (up, down)[n]), device_id_type=MESH)

    when_each([up_earlier, down_earlier], answer_rim)

    loads[0].wait()
    own = owners[...]
    hot = (lax.broadcasted_iota(jnp.int32, (regions, tile_dev), 0) == own).astype(F32)
    before = (lax.broadcasted_iota(jnp.int32, (tile_dev, tile_dev), 0)
              < lax.broadcasted_iota(jnp.int32, (tile_dev, tile_dev), 1)).astype(F32)
    count = jnp.dot(hot.astype(BF16), before.astype(BF16), preferred_element_type=F32)
    rank = jnp.sum(hot * count, axis=0, keepdims=True).astype(jnp.int32)
    place = own * 8 + rank
    pick = (lax.broadcasted_iota(jnp.int32, (8 * regions, tile_dev), 0) == place).astype(F32)
    pick3 = jnp.concatenate([pick, pick, pick], axis=1).astype(BF16)
    for load in loads[1:4]:
        load.wait()
    for f in range(FIELDS):
        field = coords[f] if f < 3 else (smooth[...] if f == 3 else masses[...])
        stack = jnp.concatenate(split3(field), axis=0).astype(BF16)
        got = jnp.dot(pick3, stack, preferred_element_type=F32)
        for d in range(regions):
            packed[d, pl.ds(f, group, stride=FIELDS), :] = got[8 * d : 8 * d + group]

    copies = [pltpu.make_async_remote_copy(
        src_ref=packed.at[dst], dst_ref=landed.at[rim + r], send_sem=send_sem.at[n],
        recv_sem=recv_sem.at[r], device_id=(dst, s), device_id_type=MESH) for n, dst in enumerate(peers)]
    metas = [[
        pltpu.make_async_remote_copy(
            src_ref=src, dst_ref=dst.at[slot], send_sem=meta_send.at[2 * n + slot],
            recv_sem=meta_recv.at[2 * n + slot], device_id=(r, peer), device_id_type=MESH)
        for n, (src, dst) in enumerate(((counts_hbm, rim_counts_v), (lists_hbm, rim_lists_v)))]
        for slot, peer in enumerate((up, down))]
    rims = [
        pltpu.make_async_remote_copy(
            src_ref=landed.at[pl.ds(regions, rim)], dst_ref=landed.at[pl.ds(0, rim)],
            send_sem=rim_send.at[0], recv_sem=rim_recv.at[0], device_id=(r, up), device_id_type=MESH),
        pltpu.make_async_remote_copy(
            src_ref=landed.at[pl.ds(rim, rim)], dst_ref=landed.at[pl.ds(rim + regions, rim)],
            send_sem=rim_send.at[1], recv_sem=rim_recv.at[1], device_id=(r, down), device_id_type=MESH),
    ]

    def send_meta(slot):
        for copy in metas[slot]:
            copy.start()

    def send_rim(slot):
        rims[slot].start()

    def answered_rim(slot):
        pl.semaphore_wait(rim_ok.at[slot], 1)
        send_meta(slot)
        send_rim(slot)

    def arrived(src):
        @pl.when(src != r)
        def _():
            pltpu.make_async_remote_copy(
                src_ref=packed.at[src], dst_ref=landed.at[rim + src], send_sem=send_sem.at[0],
                recv_sem=recv_sem.at[src], device_id=(src, s), device_id_type=MESH).wait_recv()

    def answered(n):
        pl.semaphore_wait(ok.at[peers[n]], 1)
        copies[n].start()

    def send_up():
        for src in last:
            arrived(src)
        send_rim(0)

    top = RIM + tile_dev
    last = range(regions - rim, regions)
    def send_earlier(now):
        for n in reversed(range(regions)):
            pl.when(jnp.logical_and(earlier[n], now))(copies[n].start)

    ahead = r >= regions - rim
    send_earlier(ahead)
    when_each([up_earlier, down_earlier], send_meta)
    landed[rim + r] = packed[r]
    when_each(later[: regions - 2], answered)
    ends = jnp.logical_or(r < 2, r >= regions - 2)
    pl.when(jnp.logical_and(up_earlier, ends))(send_up)
    send_earlier(jnp.logical_not(ahead))
    root = s == 0
    pl.when(later[regions - 2])(functools.partial(answered, regions - 2))
    pl.when(jnp.logical_and(later[regions - 1], jnp.logical_not(root)))(functools.partial(answered, regions - 1))
    pl.when(jnp.logical_and(up_earlier, jnp.logical_not(ends)))(send_up)

    @pl.when(jnp.logical_not(up_earlier))
    def _():
        for src in last:
            arrived(src)
        answered_rim(0)

    @pl.when(down_earlier)
    def _():
        for src in range(rim):
            arrived(src)
        send_rim(1)

    lane = lax.broadcasted_iota(jnp.int32, (1, rows), 1)
    for load in loads[4:]:
        load.wait()

    def live_step(t, carry):
        live[pl.ds(t + RIM, 1), :] = (lane < counts[0, t]).astype(F32)
        return carry

    lax.fori_loop(0, tile_dev, live_step, 0, unroll=UNROLL)
    for src in range(rim, regions - rim):
        arrived(src)

    @pl.when(jnp.logical_not(down_earlier))
    def _():
        for src in range(1, rim):
            arrived(src)

    pl.when(jnp.logical_and(later[regions - 1], root))(functools.partial(answered, regions - 1))

    def unpack(groups):
        for g in groups:
            for f in range(FIELDS):
                fields[f, group * g : group * (g + 1), :] = landed[g, pl.ds(f, group, stride=FIELDS), :]

    def pair_features(a, b):
        x, y, z, h, m = (fields[f, a:b, :] for f in range(FIELDS))
        norm_sq = x * x + y * y + z * z
        zero, one = jnp.zeros_like(x), jnp.ones_like(x)
        mass_log2 = jnp.where(live[a:b, :] > 0, jnp.log2(m), DEAD_LOG2)
        scale = LOG2E / (h * h)
        own_const = NORM_LOG2 - 3.0 * jnp.log2(h) - scale * norm_sq
        twice = 2.0 * scale
        for k, v in enumerate((x, y, z, norm_sq, one, mass_log2, zero, zero)):
            partner8[pl.ds(8 * a + k, b - a, stride=8), :] = v
        for k, v in enumerate((twice * x, twice * y, twice * z, -scale, own_const, one, zero, zero)):
            own8[pl.ds(8 * a + k, b - a, stride=8), :] = v

        def partner_step(e, carry):
            hi, mid, lo = split3(partner8[pl.ds(pl.multiple_of(e * 8, 8), 8), :])
            partner_t[e] = jnp.concatenate([hi, mid, hi, mid, lo, hi], axis=0).T.astype(BF16)
            return carry

        lax.fori_loop(a, b, partner_step, 0, unroll=largest(b - a))

    def density_of(e, partners, slot):
        hi, mid, lo = split3(own8[pl.ds(pl.multiple_of(e * 8, 8), 8), :])
        mine = jnp.concatenate([hi, hi, mid, mid, hi, lo], axis=0).astype(BF16)
        total = None
        for nb, partner in enumerate(partners):
            w = jnp.exp2(jnp.dot(partner_t[partner], mine, preferred_element_type=F32))
            part = jnp.sum(w.reshape(rows // 8, 8, rows), axis=0)
            total = part if total is None else total + part
            if slot is not None:
                high = w.astype(BF16)
                weight_hi[slot, nb * rows : (nb + 1) * rows, :] = high
                weight_lo[slot, nb * rows : (nb + 1) * rows, :] = (w - high.astype(F32)).astype(BF16)
        raw[pl.ds(e, 1), :] = jnp.sum(total, axis=0, keepdims=True)

    def own_partners(t):
        return [lists[nb, t] + HALO for nb in range(4)]

    def pressures(a, b):
        alive = live[a:b, :] > 0
        total = jnp.where(alive, raw[a:b, :], 1.0)
        return jnp.where(alive, jnp.exp2(jnp.log2(total) * (-1.0 / 3.0)), 0.0)

    def force_features(a, b):
        q = pressures(a, b)
        x, y, z = (fields[f, a:b, :] for f in range(3))
        for k, v in enumerate((jnp.ones_like(q), x, y, z, q, q * x, q * y, q * z)):
            force8[pl.ds(8 * a + k, b - a, stride=8), :] = v

        def step(e, carry):
            v = force8[pl.ds(pl.multiple_of(e * 8, 8), 8), :]
            hi = v.astype(BF16).astype(F32)
            force_f[e] = jnp.concatenate([hi, v - hi], axis=0).astype(BF16)
            return carry

        lax.fori_loop(a, b, step, 0, unroll=largest(b - a))

    def force_of(t):
        feats = jnp.concatenate([force_f[p] for p in own_partners(t)], axis=1)
        got = (jnp.dot(feats, weight_hi[t], preferred_element_type=F32)
               + jnp.dot(feats, weight_lo[t], preferred_element_type=F32))
        sums8[pl.ds(pl.multiple_of(t * 8, 8), 8), :] = got[:8] + got[8:]

    def finish(a, b):
        alive = live[RIM + a : RIM + b, :] > 0
        q = pressures(RIM + a, RIM + b)
        h = fields[3, RIM + a : RIM + b, :]
        density_ref[a:b, :] = jnp.where(alive, raw[RIM + a : RIM + b, :], 0.0)
        plain, pressed = (sums8[pl.ds(8 * a + k, b - a, stride=8), :] for k in (0, 4))
        both = q * plain + pressed
        factor = jnp.where(alive, 2.0 / (h * h), 0.0)
        for k in range(3):
            near, far = (sums8[pl.ds(8 * a + j + k, b - a, stride=8), :] for j in (1, 5))
            accel_ref[k, a:b, :] = factor * (fields[k, RIM + a : RIM + b, :] * both - (q * near + far))

    def inner_density(t, carry):
        density_of(t + RIM, own_partners(t), t)
        return carry

    def inner_force(t, carry):
        force_of(t)
        return carry

    unpack(range(rim + 1, rim + regions))
    pair_features(RIM + group, top)
    low = group + HALO
    lax.fori_loop(low, tile_dev - HALO, inner_density, 0, unroll=largest(tile_dev - HALO - low))
    force_features(RIM + low, top)
    lax.fori_loop(low + HALO, tile_dev - RIM, inner_force, 0, unroll=largest(tile_dev - RIM - low - HALO))

    @pl.when(jnp.logical_not(down_earlier))
    def _():
        arrived(0)
        answered_rim(1)


    for copy in metas[0] + metas[1]:
        copy.wait_recv()
    moves = [pltpu.make_async_copy(rim_counts_v, rim_counts, meta_sem.at[0]),
             pltpu.make_async_copy(rim_lists_v, rim_lists, meta_sem.at[1])]
    for move in moves:
        move.start()
    for move in moves:
        move.wait()
    for k in range(RIM):
        live[k : k + 1, :] = (lane < rim_counts[0, 0, tile_dev - RIM + k]).astype(F32)
        live[top + k : top + k + 1, :] = (lane < rim_counts[1, 0, k]).astype(F32)

    rims[1].wait_recv()
    unpack([rim] + list(range(rim + regions, 2 * rim + regions)))
    pair_features(RIM, RIM + group)
    pair_features(top, top + RIM)
    for t in range(HALO, low):
        density_of(RIM + t, own_partners(t), t)
    for k in range(HALO):
        density_of(top - HALO + k, own_partners(tile_dev - HALO + k), tile_dev - HALO + k)
        above = [rim_lists[1, nb, k] + (HALO + tile_dev) for nb in range(4)]
        density_of(top + k, above, None)
    force_features(RIM + HALO, RIM + low)
    force_features(top - RIM, top + RIM)
    for t in list(range(RIM, low + HALO)) + list(range(tile_dev - RIM, tile_dev)):
        force_of(t)
    finish(RIM, tile_dev)

    rims[0].wait_recv()
    unpack(range(rim))
    pair_features(0, RIM)
    for k in range(HALO):
        below = [jnp.maximum(rim_lists[0, nb, tile_dev - HALO + k] + (HALO - tile_dev), 0) for nb in range(4)]
        density_of(HALO + k, below, None)
        density_of(RIM + k, own_partners(k), k)
    force_features(0, 2 * RIM)
    for k in range(RIM):
        force_of(k)
    finish(0, RIM)
    when_each([mine != k for k in range(regions)], lambda n: copies[n].wait_send())
    for copy in metas[0] + metas[1] + rims:
        copy.wait_send()


def per_device(coords, smooth, masses, owners, counts, neighbours):
    regions, subs = lax.axis_size("region"), lax.axis_size("sub")
    tile_dev, rows = smooth.shape
    group = tile_dev // regions
    groups = regions + 2 * (RIM // group)
    ext = tile_dev + 2 * RIM
    owners, counts, lists = owners.reshape(1, -1), counts.reshape(1, -1), neighbours.T
    vmem = pl.BlockSpec(memory_space=pltpu.VMEM)
    dma = pltpu.SemaphoreType.DMA
    return pl.pallas_call(
        functools.partial(kernel, regions, subs),
        out_shape=(pltpu.VMEM((tile_dev, rows), F32), pltpu.VMEM((3, tile_dev, rows), F32)),
        in_specs=[pl.BlockSpec(memory_space=pl.ANY)] * 6,
        out_specs=(vmem, vmem),
        scratch_shapes=[
            pltpu.VMEM(coords.shape, F32), pltpu.VMEM(smooth.shape, F32), pltpu.VMEM(masses.shape, F32),
            pltpu.VMEM(owners.shape, jnp.int32),
            pltpu.SMEM(counts.shape, jnp.int32), pltpu.SMEM(lists.shape, jnp.int32),
            pltpu.VMEM((2,) + counts.shape, jnp.int32), pltpu.VMEM((2,) + lists.shape, jnp.int32),
            pltpu.SMEM((2,) + counts.shape, jnp.int32), pltpu.SMEM((2,) + lists.shape, jnp.int32),
            pltpu.VMEM((regions, group * FIELDS, rows), F32),
            pltpu.VMEM((groups, group * FIELDS, rows), F32),
            pltpu.VMEM((FIELDS, ext, rows), F32),
            pltpu.VMEM((ext, rows), F32),
            pltpu.VMEM((ext * 8, rows), F32),
            pltpu.VMEM((ext * 8, rows), F32),
            pltpu.VMEM((ext, rows, 48), BF16),
            pltpu.VMEM((tile_dev, 4 * rows, rows), BF16),
            pltpu.VMEM((tile_dev, 4 * rows, rows), BF16),
            pltpu.VMEM((ext, rows), F32),
            pltpu.VMEM((ext * 8, rows), F32),
            pltpu.VMEM((ext, 16, rows), BF16),
            pltpu.VMEM((tile_dev * 8, rows), F32),
            dma((6,)), dma((regions,)), dma((regions,)), dma((2,)), dma((2,)), dma((4,)), dma((4,)), dma((2,)),
            pltpu.SemaphoreType.REGULAR((regions,)), pltpu.SemaphoreType.REGULAR((2,)),
        ],
        compiler_params=pltpu.CompilerParams(collective_id=0, has_side_effects=True),
        name="sph",
    )(coords, smooth, masses, owners, counts, lists)


def solution(mesh):
    rs = ("region", "sub")
    in_specs = (P(None, rs, None), P(rs, None), P(rs, None), P(rs), P(rs), P(rs, None))
    out_specs = (P(rs, None), P(None, rs, None))
    return jax.shard_map(per_device, mesh=mesh, in_specs=in_specs, out_specs=out_specs, check_vma=False)
```

```python
import functools
import math

import jax
import jax.numpy as jnp
from jax import lax
from jax.experimental import pallas as pl
from jax.experimental.pallas import tpu as pltpu
from jax.sharding import PartitionSpec as P

HALO = 4
RIM = 2 * HALO
FIELDS = 5
UNROLL = 8
DIRECT = 8
SUB_RUN = 12
LOG2E = math.log2(math.e)
NORM_LOG2 = -1.5 * math.log2(math.pi)
DEAD_LOG2 = -1000.0
MESH = pl.DeviceIdType.MESH
F32 = jnp.float32
BF16 = jnp.bfloat16


def largest(n, most=13):
    return max(k for k in range(1, most + 1) if n % k == 0)


def split3(v):
    hi = v.astype(BF16).astype(F32)
    rest = v - hi
    mid = rest.astype(BF16).astype(F32)
    return hi, mid, rest - mid


def kernel(regions, subs, coords_hbm, smooth_hbm, masses_hbm, owners_hbm, counts_hbm, lists_hbm,
           density_ref, accel_ref,
           coords, smooth, masses, owners, counts, lists, rim_counts_v, rim_lists_v, rim_counts, rim_lists,
           packed, landed, fields, live, partner8, own8, partner_t, weight_hi, weight_lo, raw, force8, force_f, sums8,
           in_sem, send_sem, recv_sem, rim_send, rim_recv, meta_send, meta_recv, meta_sem, ok, rim_ok,
           direct_send, direct_recv):
    tile_dev, rows = smooth.shape
    group = tile_dev // regions
    rim = RIM // group
    r = lax.axis_index("region")
    s = lax.axis_index("sub")
    up = lax.rem(s + 1, subs)
    down = lax.rem(s + subs - 1, subs)

    run = lax.rem(s, SUB_RUN) if subs % SUB_RUN == 0 else s
    last_run = (SUB_RUN if subs % SUB_RUN == 0 else subs) - 1
    down_earlier = run > 0
    up_earlier = run == last_run

    def partner(k):
        chips = regions // 2

        def at(k):
            y = k // 2
            return 2 * (y if y < chips // 2 else chips + chips // 2 - 1 - y) + k % 2

        return jnp.where(s == 0, 0 if k == regions - 1 else at(k + 1), at(k))

    def order(i):
        chips = regions // 2
        y = i // 2
        place = 2 * jnp.where(y < chips // 2, y, chips + chips // 2 - 1 - y) + lax.rem(i, 2)
        return jnp.where(s == 0, jnp.where(i == 0, regions - 1, place - 1), place)

    mine = order(r)
    peers = [partner(k) for k in range(regions)]
    later = [mine < k for k in range(regions)]
    earlier = [mine > k for k in range(regions)]

    def when_each(conditions, action):
        for n, condition in enumerate(conditions):
            pl.when(condition)(functools.partial(action, n))

    barrier = pltpu.get_barrier_semaphore()

    def greet(n):
        pl.semaphore_signal(barrier, inc=1, device_id=(peers[n], s), device_id_type=MESH)

    when_each(later, greet)

    def greet_rim(n):
        pl.semaphore_signal(barrier, inc=1, device_id=(r, (up, down)[n]), device_id_type=MESH)

    when_each([jnp.logical_not(up_earlier), jnp.logical_not(down_earlier)], greet_rim)
    ahead = r >= regions - rim
    gets_direct = jnp.logical_and(jnp.logical_not(down_earlier), r < DIRECT)
    skips_rim = jnp.logical_and(up_earlier, r < DIRECT)
    gives_direct = jnp.logical_and(up_earlier, ahead)

    @pl.when(gets_direct)
    def _():
        for g in range(regions - rim, regions):
            pl.semaphore_signal(barrier, inc=1, device_id=(g, down), device_id_type=MESH)

    loads = [pltpu.make_async_copy(src, dst, in_sem.at[n]) for n, (src, dst) in enumerate((
        (owners_hbm, owners), (coords_hbm, coords), (smooth_hbm, smooth), (masses_hbm, masses),
        (counts_hbm, counts), (lists_hbm, lists)))]
    for load in loads:
        load.start()
    expected = mine + down_earlier.astype(jnp.int32) + up_earlier.astype(jnp.int32) + jnp.where(gives_direct, DIRECT, 0)

    @pl.when(expected > 0)
    def _():
        pl.semaphore_wait(barrier, expected)

    def answer(n):
        pl.semaphore_signal(ok.at[r], inc=1, device_id=(peers[n], s), device_id_type=MESH)

    when_each(earlier, answer)

    def answer_rim(n):
        pl.semaphore_signal(rim_ok.at[1 - n], inc=1, device_id=(r, (up, down)[n]), device_id_type=MESH)

    when_each([up_earlier, down_earlier], answer_rim)

    loads[0].wait()
    own = owners[...]
    hot = (lax.broadcasted_iota(jnp.int32, (regions, tile_dev), 0) == own).astype(F32)
    before = (lax.broadcasted_iota(jnp.int32, (tile_dev, tile_dev), 0)
              < lax.broadcasted_iota(jnp.int32, (tile_dev, tile_dev), 1)).astype(F32)
    count = jnp.dot(hot.astype(BF16), before.astype(BF16), preferred_element_type=F32)
    rank = jnp.sum(hot * count, axis=0, keepdims=True).astype(jnp.int32)
    place = own * 8 + rank
    pick = (lax.broadcasted_iota(jnp.int32, (8 * regions, tile_dev), 0) == place).astype(F32)
    pick3 = jnp.concatenate([pick, pick, pick], axis=1).astype(BF16)
    for load in loads[1:4]:
        load.wait()
    for f in range(FIELDS):
        field = coords[f] if f < 3 else (smooth[...] if f == 3 else masses[...])
        stack = jnp.concatenate(split3(field), axis=0).astype(BF16)
        got = jnp.dot(pick3, stack, preferred_element_type=F32)
        for d in range(regions):
            packed[d, pl.ds(f, group, stride=FIELDS), :] = got[8 * d : 8 * d + group]

    copies = [pltpu.make_async_remote_copy(
        src_ref=packed.at[dst], dst_ref=landed.at[rim + r], send_sem=send_sem.at[n],
        recv_sem=recv_sem.at[r], device_id=(dst, s), device_id_type=MESH) for n, dst in enumerate(peers)]
    metas = [[
        pltpu.make_async_remote_copy(
            src_ref=src, dst_ref=dst.at[slot], send_sem=meta_send.at[2 * n + slot],
            recv_sem=meta_recv.at[2 * n + slot], device_id=(r, peer), device_id_type=MESH)
        for n, (src, dst) in enumerate(((counts_hbm, rim_counts_v), (lists_hbm, rim_lists_v)))]
        for slot, peer in enumerate((up, down))]
    rims = [
        pltpu.make_async_remote_copy(
            src_ref=landed.at[pl.ds(regions, rim)], dst_ref=landed.at[pl.ds(0, rim)],
            send_sem=rim_send.at[0], recv_sem=rim_recv.at[0], device_id=(r, up), device_id_type=MESH),
        pltpu.make_async_remote_copy(
            src_ref=landed.at[pl.ds(rim, rim)], dst_ref=landed.at[pl.ds(rim + regions, rim)],
            send_sem=rim_send.at[1], recv_sem=rim_recv.at[1], device_id=(r, down), device_id_type=MESH),
    ]

    def send_meta(slot):
        for copy in metas[slot]:
            copy.start()

    def send_rim(slot):
        rims[slot].start()

    def answered_rim(slot):
        pl.semaphore_wait(rim_ok.at[slot], 1)
        send_meta(slot)
        send_rim(slot)

    def arrived(src):
        @pl.when(src != r)
        def _():
            pltpu.make_async_remote_copy(
                src_ref=packed.at[src], dst_ref=landed.at[rim + src], send_sem=send_sem.at[0],
                recv_sem=recv_sem.at[src], device_id=(src, s), device_id_type=MESH).wait_recv()

    def answered(n):
        pl.semaphore_wait(ok.at[peers[n]], 1)
        copies[n].start()

    def send_up():
        for src in last:
            arrived(src)
        pl.when(jnp.logical_not(skips_rim))(functools.partial(send_rim, 0))

    top = RIM + tile_dev
    last = range(regions - rim, regions)
    def send_earlier(now):
        for n in reversed(range(regions)):
            pl.when(jnp.logical_and(earlier[n], now))(copies[n].start)

    direct = [pltpu.make_async_remote_copy(
        src_ref=packed.at[d], dst_ref=landed.at[r - (regions - rim)], send_sem=direct_send.at[d],
        recv_sem=direct_recv.at[r - (regions - rim)], device_id=(d, up), device_id_type=MESH) for d in range(DIRECT)]

    @pl.when(gives_direct)
    def _():
        for copy in direct:
            copy.start()

    send_earlier(ahead)
    when_each([up_earlier, down_earlier], send_meta)
    landed[rim + r] = packed[r]
    when_each(later[: regions - 2], answered)
    ends = jnp.logical_or(r < 2, r >= regions - 2)
    pl.when(jnp.logical_and(up_earlier, ends))(send_up)
    send_earlier(jnp.logical_not(ahead))
    root = s == 0
    pl.when(later[regions - 2])(functools.partial(answered, regions - 2))
    pl.when(jnp.logical_and(later[regions - 1], jnp.logical_not(root)))(functools.partial(answered, regions - 1))
    pl.when(jnp.logical_and(up_earlier, jnp.logical_not(ends)))(send_up)

    @pl.when(jnp.logical_not(up_earlier))
    def _():
        for src in last:
            arrived(src)
        answered_rim(0)

    @pl.when(down_earlier)
    def _():
        for src in range(rim):
            arrived(src)
        send_rim(1)

    lane = lax.broadcasted_iota(jnp.int32, (1, rows), 1)
    for load in loads[4:]:
        load.wait()

    def live_step(t, carry):
        live[pl.ds(t + RIM, 1), :] = (lane < counts[0, t]).astype(F32)
        return carry

    lax.fori_loop(0, tile_dev, live_step, 0, unroll=UNROLL)
    for src in range(rim, regions - rim):
        arrived(src)

    @pl.when(jnp.logical_not(down_earlier))
    def _():
        for src in range(1, rim):
            arrived(src)

    pl.when(jnp.logical_and(later[regions - 1], root))(functools.partial(answered, regions - 1))

    def unpack(groups):
        for g in groups:
            for f in range(FIELDS):
                fields[f, group * g : group * (g + 1), :] = landed[g, pl.ds(f, group, stride=FIELDS), :]

    def pair_features(a, b):
        x, y, z, h, m = (fields[f, a:b, :] for f in range(FIELDS))
        norm_sq = x * x + y * y + z * z
        zero, one = jnp.zeros_like(x), jnp.ones_like(x)
        mass_log2 = jnp.where(live[a:b, :] > 0, jnp.log2(m), DEAD_LOG2)
        scale = LOG2E / (h * h)
        own_const = NORM_LOG2 - 3.0 * jnp.log2(h) - scale * norm_sq
        twice = 2.0 * scale
        for k, v in enumerate((x, y, z, norm_sq, one, mass_log2, zero, zero)):
            partner8[pl.ds(8 * a + k, b - a, stride=8), :] = v
        for k, v in enumerate((twice * x, twice * y, twice * z, -scale, own_const, one, zero, zero)):
            own8[pl.ds(8 * a + k, b - a, stride=8), :] = v

        def partner_step(e, carry):
            hi, mid, lo = split3(partner8[pl.ds(pl.multiple_of(e * 8, 8), 8), :])
            partner_t[e] = jnp.concatenate([hi, mid, hi, mid, lo, hi], axis=0).T.astype(BF16)
            return carry

        lax.fori_loop(a, b, partner_step, 0, unroll=largest(b - a))

    def density_of(e, partners, slot):
        hi, mid, lo = split3(own8[pl.ds(pl.multiple_of(e * 8, 8), 8), :])
        mine = jnp.concatenate([hi, hi, mid, mid, hi, lo], axis=0).astype(BF16)
        total = None
        for nb, partner in enumerate(partners):
            w = jnp.exp2(jnp.dot(partner_t[partner], mine, preferred_element_type=F32))
            part = jnp.sum(w.reshape(rows // 8, 8, rows), axis=0)
            total = part if total is None else total + part
            if slot is not None:
                high = w.astype(BF16)
                weight_hi[slot, nb * rows : (nb + 1) * rows, :] = high
                weight_lo[slot, nb * rows : (nb + 1) * rows, :] = (w - high.astype(F32)).astype(BF16)
        raw[pl.ds(e, 1), :] = jnp.sum(total, axis=0, keepdims=True)

    def own_partners(t):
        return [lists[nb, t] + HALO for nb in range(4)]

    def pressures(a, b):
        alive = live[a:b, :] > 0
        total = jnp.where(alive, raw[a:b, :], 1.0)
        return jnp.where(alive, jnp.exp2(jnp.log2(total) * (-1.0 / 3.0)), 0.0)

    def force_features(a, b):
        q = pressures(a, b)
        x, y, z = (fields[f, a:b, :] for f in range(3))
        for k, v in enumerate((jnp.ones_like(q), x, y, z, q, q * x, q * y, q * z)):
            force8[pl.ds(8 * a + k, b - a, stride=8), :] = v

        def step(e, carry):
            v = force8[pl.ds(pl.multiple_of(e * 8, 8), 8), :]
            hi = v.astype(BF16).astype(F32)
            force_f[e] = jnp.concatenate([hi, v - hi], axis=0).astype(BF16)
            return carry

        lax.fori_loop(a, b, step, 0, unroll=largest(b - a))

    def force_of(t):
        feats = jnp.concatenate([force_f[p] for p in own_partners(t)], axis=1)
        got = (jnp.dot(feats, weight_hi[t], preferred_element_type=F32)
               + jnp.dot(feats, weight_lo[t], preferred_element_type=F32))
        sums8[pl.ds(pl.multiple_of(t * 8, 8), 8), :] = got[:8] + got[8:]

    def finish(a, b):
        alive = live[RIM + a : RIM + b, :] > 0
        q = pressures(RIM + a, RIM + b)
        h = fields[3, RIM + a : RIM + b, :]
        density_ref[a:b, :] = jnp.where(alive, raw[RIM + a : RIM + b, :], 0.0)
        plain, pressed = (sums8[pl.ds(8 * a + k, b - a, stride=8), :] for k in (0, 4))
        both = q * plain + pressed
        factor = jnp.where(alive, 2.0 / (h * h), 0.0)
        for k in range(3):
            near, far = (sums8[pl.ds(8 * a + j + k, b - a, stride=8), :] for j in (1, 5))
            accel_ref[k, a:b, :] = factor * (fields[k, RIM + a : RIM + b, :] * both - (q * near + far))

    def inner_density(t, carry):
        density_of(t + RIM, own_partners(t), t)
        return carry

    def inner_force(t, carry):
        force_of(t)
        return carry

    unpack(range(rim + 1, rim + regions))
    pair_features(RIM + group, top)
    low = group + HALO
    lax.fori_loop(low, tile_dev - HALO, inner_density, 0, unroll=largest(tile_dev - HALO - low))
    force_features(RIM + low, top)
    lax.fori_loop(low + HALO, tile_dev - RIM, inner_force, 0, unroll=largest(tile_dev - RIM - low - HALO))

    @pl.when(jnp.logical_not(down_earlier))
    def _():
        arrived(0)
        answered_rim(1)


    for copy in metas[0] + metas[1]:
        copy.wait_recv()
    moves = [pltpu.make_async_copy(rim_counts_v, rim_counts, meta_sem.at[0]),
             pltpu.make_async_copy(rim_lists_v, rim_lists, meta_sem.at[1])]
    for move in moves:
        move.start()
    for move in moves:
        move.wait()
    for k in range(RIM):
        live[k : k + 1, :] = (lane < rim_counts[0, 0, tile_dev - RIM + k]).astype(F32)
        live[top + k : top + k + 1, :] = (lane < rim_counts[1, 0, k]).astype(F32)

    rims[1].wait_recv()
    unpack([rim] + list(range(rim + regions, 2 * rim + regions)))
    pair_features(RIM, RIM + group)
    pair_features(top, top + RIM)
    for t in range(HALO, low):
        density_of(RIM + t, own_partners(t), t)
    for k in range(HALO):
        density_of(top - HALO + k, own_partners(tile_dev - HALO + k), tile_dev - HALO + k)
        above = [rim_lists[1, nb, k] + (HALO + tile_dev) for nb in range(4)]
        density_of(top + k, above, None)
    force_features(RIM + HALO, RIM + low)
    force_features(top - RIM, top + RIM)
    for t in list(range(RIM, low + HALO)) + list(range(tile_dev - RIM, tile_dev)):
        force_of(t)
    finish(RIM, tile_dev)

    pl.when(jnp.logical_not(gets_direct))(rims[0].wait_recv)

    @pl.when(gets_direct)
    def _():
        for g in range(rim):
            pltpu.make_async_remote_copy(
                src_ref=packed.at[g], dst_ref=landed.at[g], send_sem=direct_send.at[0],
                recv_sem=direct_recv.at[g], device_id=(r, down), device_id_type=MESH).wait_recv()

    unpack(range(rim))
    pair_features(0, RIM)
    for k in range(HALO):
        below = [jnp.maximum(rim_lists[0, nb, tile_dev - HALO + k] + (HALO - tile_dev), 0) for nb in range(4)]
        density_of(HALO + k, below, None)
        density_of(RIM + k, own_partners(k), k)
    force_features(0, 2 * RIM)
    for k in range(RIM):
        force_of(k)
    finish(0, RIM)
    when_each([mine != k for k in range(regions)], lambda n: copies[n].wait_send())
    pl.when(jnp.logical_not(skips_rim))(rims[0].wait_send)

    @pl.when(gives_direct)
    def _():
        for copy in direct:
            copy.wait_send()

    for copy in metas[0] + metas[1] + rims[1:]:
        copy.wait_send()


def store_kernel(density, accel, density_hbm, accel_hbm, sem):
    copies = [pltpu.make_async_copy(density, density_hbm, sem.at[0]), pltpu.make_async_copy(accel, accel_hbm, sem.at[1])]
    for copy in copies:
        copy.start()
    for copy in copies:
        copy.wait()


def per_device(coords, smooth, masses, owners, counts, neighbours):
    regions, subs = lax.axis_size("region"), lax.axis_size("sub")
    tile_dev, rows = smooth.shape
    group = tile_dev // regions
    rim = RIM // group
    groups = regions + 2 * rim
    ext = tile_dev + 2 * RIM
    owners, counts, lists = owners.reshape(1, -1), counts.reshape(1, -1), neighbours.T
    vmem = pl.BlockSpec(memory_space=pltpu.VMEM)
    dma = pltpu.SemaphoreType.DMA
    density, accel = pl.pallas_call(
        functools.partial(kernel, regions, subs),
        out_shape=(pltpu.VMEM((tile_dev, rows), F32), pltpu.VMEM((3, tile_dev, rows), F32)),
        in_specs=[pl.BlockSpec(memory_space=pl.ANY)] * 6,
        out_specs=(vmem, vmem),
        scratch_shapes=[
            pltpu.VMEM(coords.shape, F32), pltpu.VMEM(smooth.shape, F32), pltpu.VMEM(masses.shape, F32),
            pltpu.VMEM(owners.shape, jnp.int32),
            pltpu.SMEM(counts.shape, jnp.int32), pltpu.SMEM(lists.shape, jnp.int32),
            pltpu.VMEM((2,) + counts.shape, jnp.int32), pltpu.VMEM((2,) + lists.shape, jnp.int32),
            pltpu.SMEM((2,) + counts.shape, jnp.int32), pltpu.SMEM((2,) + lists.shape, jnp.int32),
            pltpu.VMEM((regions, group * FIELDS, rows), F32),
            pltpu.VMEM((groups, group * FIELDS, rows), F32),
            pltpu.VMEM((FIELDS, ext, rows), F32),
            pltpu.VMEM((ext, rows), F32),
            pltpu.VMEM((ext * 8, rows), F32),
            pltpu.VMEM((ext * 8, rows), F32),
            pltpu.VMEM((ext, rows, 48), BF16),
            pltpu.VMEM((tile_dev, 4 * rows, rows), BF16),
            pltpu.VMEM((tile_dev, 4 * rows, rows), BF16),
            pltpu.VMEM((ext, rows), F32),
            pltpu.VMEM((ext * 8, rows), F32),
            pltpu.VMEM((ext, 16, rows), BF16),
            pltpu.VMEM((tile_dev * 8, rows), F32),
            dma((6,)), dma((regions,)), dma((regions,)), dma((2,)), dma((2,)), dma((4,)), dma((4,)), dma((2,)),
            pltpu.SemaphoreType.REGULAR((regions,)), pltpu.SemaphoreType.REGULAR((2,)),
            dma((DIRECT,)), dma((rim,)),
        ],
        compiler_params=pltpu.CompilerParams(collective_id=0, has_side_effects=True),
        name="sph",
    )(coords, smooth, masses, owners, counts, lists)
    return pl.pallas_call(
        store_kernel,
        out_shape=(jax.ShapeDtypeStruct(density.shape, F32), jax.ShapeDtypeStruct(accel.shape, F32)),
        in_specs=[pl.BlockSpec(memory_space=pl.ANY)] * 2,
        out_specs=[pl.BlockSpec(memory_space=pl.ANY)] * 2,
        scratch_shapes=[dma((2,))],
        name="store",
    )(*(pltpu.with_memory_space_constraint(v, pltpu.VMEM) for v in (density, accel)))


def solution(mesh):
    rs = ("region", "sub")
    in_specs = (P(None, rs, None), P(rs, None), P(rs, None), P(rs), P(rs), P(rs, None))
    out_specs = (P(rs, None), P(None, rs, None))
    return jax.shard_map(per_device, mesh=mesh, in_specs=in_specs, out_specs=out_specs, check_vma=False)
```

```python
import functools
import math

import jax
import jax.numpy as jnp
from jax import lax
from jax.experimental import pallas as pl
from jax.experimental.pallas import tpu as pltpu
from jax.sharding import PartitionSpec as P

HALO = 4
RIM = 2 * HALO
FIELDS = 5
UNROLL = 8
DIRECT = 8
SUB_RUN = 12
LOG2E = math.log2(math.e)
NORM_LOG2 = -1.5 * math.log2(math.pi)
DEAD_LOG2 = -1000.0
MESH = pl.DeviceIdType.MESH
F32 = jnp.float32
BF16 = jnp.bfloat16


def largest(n, most=13):
    return max(k for k in range(1, most + 1) if n % k == 0)


def split3(v):
    hi = v.astype(BF16).astype(F32)
    rest = v - hi
    mid = rest.astype(BF16).astype(F32)
    return hi, mid, rest - mid


def kernel(regions, subs, coords_hbm, smooth_hbm, masses_hbm, owners_hbm, counts_hbm, lists_hbm,
           density_ref, accel_ref,
           coords, smooth, masses, owners, counts, lists, rim_counts_v, rim_lists_v, rim_counts, rim_lists,
           packed, landed, fields, live, partner8, own8, partner_t, weight_hi, weight_lo, raw, force8, force_f, sums8,
           in_sem, send_sem, recv_sem, rim_send, rim_recv, meta_send, meta_recv, meta_sem, ok, rim_ok,
           direct_send, direct_recv):
    tile_dev, rows = smooth.shape
    group = tile_dev // regions
    rim = RIM // group
    r = lax.axis_index("region")
    s = lax.axis_index("sub")
    up = lax.rem(s + 1, subs)
    down = lax.rem(s + subs - 1, subs)

    run = lax.rem(s, SUB_RUN) if subs % SUB_RUN == 0 else s
    last_run = (SUB_RUN if subs % SUB_RUN == 0 else subs) - 1
    down_earlier = run > 0
    up_earlier = run == last_run

    def partner(k):
        chips = regions // 2

        def at(k):
            y = k // 2
            return 2 * (y if y < chips // 2 else chips + chips // 2 - 1 - y) + k % 2

        return jnp.where(s == 0, 0 if k == regions - 1 else at(k + 1), at(k))

    def order(i):
        chips = regions // 2
        y = i // 2
        place = 2 * jnp.where(y < chips // 2, y, chips + chips // 2 - 1 - y) + lax.rem(i, 2)
        return jnp.where(s == 0, jnp.where(i == 0, regions - 1, place - 1), place)

    mine = order(r)
    peers = [partner(k) for k in range(regions)]
    later = [mine < k for k in range(regions)]
    earlier = [mine > k for k in range(regions)]

    def when_each(conditions, action):
        for n, condition in enumerate(conditions):
            pl.when(condition)(functools.partial(action, n))

    barrier = pltpu.get_barrier_semaphore()

    def greet(n):
        pl.semaphore_signal(barrier, inc=1, device_id=(peers[n], s), device_id_type=MESH)

    when_each(later, greet)

    def greet_rim(n):
        pl.semaphore_signal(barrier, inc=1, device_id=(r, (up, down)[n]), device_id_type=MESH)

    when_each([jnp.logical_not(up_earlier), jnp.logical_not(down_earlier)], greet_rim)
    ahead = r >= regions - rim
    gets_direct = jnp.logical_and(jnp.logical_not(down_earlier), r < DIRECT)
    skips_rim = jnp.logical_and(up_earlier, r < DIRECT)
    gives_direct = jnp.logical_and(up_earlier, ahead)

    @pl.when(gets_direct)
    def _():
        for g in range(regions - rim, regions):
            pl.semaphore_signal(barrier, inc=1, device_id=(g, down), device_id_type=MESH)

    loads = [pltpu.make_async_copy(src, dst, in_sem.at[n]) for n, (src, dst) in enumerate((
        (owners_hbm, owners), (coords_hbm, coords), (smooth_hbm, smooth), (masses_hbm, masses),
        (counts_hbm, counts), (lists_hbm, lists)))]
    for load in loads:
        load.start()
    expected = mine + down_earlier.astype(jnp.int32) + up_earlier.astype(jnp.int32) + jnp.where(gives_direct, DIRECT, 0)

    @pl.when(expected > 0)
    def _():
        pl.semaphore_wait(barrier, expected)

    def answer(n):
        pl.semaphore_signal(ok.at[r], inc=1, device_id=(peers[n], s), device_id_type=MESH)

    when_each(earlier, answer)

    def answer_rim(n):
        pl.semaphore_signal(rim_ok.at[1 - n], inc=1, device_id=(r, (up, down)[n]), device_id_type=MESH)

    when_each([up_earlier, down_earlier], answer_rim)

    loads[0].wait()
    own = owners[...]
    hot = (lax.broadcasted_iota(jnp.int32, (regions, tile_dev), 0) == own).astype(F32)
    before = (lax.broadcasted_iota(jnp.int32, (tile_dev, tile_dev), 0)
              < lax.broadcasted_iota(jnp.int32, (tile_dev, tile_dev), 1)).astype(F32)
    count = jnp.dot(hot.astype(BF16), before.astype(BF16), preferred_element_type=F32)
    rank = jnp.sum(hot * count, axis=0, keepdims=True).astype(jnp.int32)
    place = own * 8 + rank
    pick = (lax.broadcasted_iota(jnp.int32, (8 * regions, tile_dev), 0) == place).astype(F32)
    pick3 = jnp.concatenate([pick, pick, pick], axis=1).astype(BF16)
    for load in loads[1:4]:
        load.wait()
    for f in range(FIELDS):
        field = coords[f] if f < 3 else (smooth[...] if f == 3 else masses[...])
        stack = jnp.concatenate(split3(field), axis=0).astype(BF16)
        got = jnp.dot(pick3, stack, preferred_element_type=F32)
        for d in range(regions):
            packed[d, pl.ds(f, group, stride=FIELDS), :] = got[8 * d : 8 * d + group]

    copies = [pltpu.make_async_remote_copy(
        src_ref=packed.at[dst], dst_ref=landed.at[rim + r], send_sem=send_sem.at[n],
        recv_sem=recv_sem.at[r], device_id=(dst, s), device_id_type=MESH) for n, dst in enumerate(peers)]
    metas = [[
        pltpu.make_async_remote_copy(
            src_ref=src, dst_ref=dst.at[slot], send_sem=meta_send.at[2 * n + slot],
            recv_sem=meta_recv.at[2 * n + slot], device_id=(r, peer), device_id_type=MESH)
        for n, (src, dst) in enumerate(((counts_hbm, rim_counts_v), (lists_hbm, rim_lists_v)))]
        for slot, peer in enumerate((up, down))]
    rims = [
        pltpu.make_async_remote_copy(
            src_ref=landed.at[pl.ds(regions, rim)], dst_ref=landed.at[pl.ds(0, rim)],
            send_sem=rim_send.at[0], recv_sem=rim_recv.at[0], device_id=(r, up), device_id_type=MESH),
        pltpu.make_async_remote_copy(
            src_ref=landed.at[pl.ds(rim, rim)], dst_ref=landed.at[pl.ds(rim + regions, rim)],
            send_sem=rim_send.at[1], recv_sem=rim_recv.at[1], device_id=(r, down), device_id_type=MESH),
    ]

    def send_meta(slot):
        for copy in metas[slot]:
            copy.start()

    def send_rim(slot):
        rims[slot].start()

    def answered_rim(slot):
        pl.semaphore_wait(rim_ok.at[slot], 1)
        send_meta(slot)
        send_rim(slot)

    def arrived(src):
        @pl.when(src != r)
        def _():
            pltpu.make_async_remote_copy(
                src_ref=packed.at[src], dst_ref=landed.at[rim + src], send_sem=send_sem.at[0],
                recv_sem=recv_sem.at[src], device_id=(src, s), device_id_type=MESH).wait_recv()

    def answered(n):
        pl.semaphore_wait(ok.at[peers[n]], 1)
        copies[n].start()

    def send_up():
        for src in last:
            arrived(src)
        pl.when(jnp.logical_not(skips_rim))(functools.partial(send_rim, 0))

    top = RIM + tile_dev
    last = range(regions - rim, regions)
    def send_earlier(now, ks):
        for n in ks:
            pl.when(jnp.logical_and(earlier[n], now))(copies[n].start)

    direct = [pltpu.make_async_remote_copy(
        src_ref=packed.at[d], dst_ref=landed.at[r - (regions - rim)], send_sem=direct_send.at[d],
        recv_sem=direct_recv.at[r - (regions - rim)], device_id=(d, up), device_id_type=MESH) for d in range(DIRECT)]

    @pl.when(gives_direct)
    def _():
        for copy in direct:
            copy.start()

    send_earlier(ahead, reversed(range(regions)))
    when_each([up_earlier, down_earlier], send_meta)
    landed[rim + r] = packed[r]
    when_each(later[: regions - 2], answered)
    ends = jnp.logical_or(r < 2, r >= regions - 2)
    pl.when(jnp.logical_and(up_earlier, ends))(send_up)
    send_earlier(jnp.logical_not(ahead), range(regions))
    root = s == 0
    pl.when(later[regions - 2])(functools.partial(answered, regions - 2))
    pl.when(jnp.logical_and(later[regions - 1], jnp.logical_not(root)))(functools.partial(answered, regions - 1))
    pl.when(jnp.logical_and(up_earlier, jnp.logical_not(ends)))(send_up)

    @pl.when(jnp.logical_not(up_earlier))
    def _():
        for src in last:
            arrived(src)
        answered_rim(0)

    @pl.when(down_earlier)
    def _():
        for src in range(rim):
            arrived(src)
        send_rim(1)

    lane = lax.broadcasted_iota(jnp.int32, (1, rows), 1)
    for load in loads[4:]:
        load.wait()

    def live_step(t, carry):
        live[pl.ds(t + RIM, 1), :] = (lane < counts[0, t]).astype(F32)
        return carry

    lax.fori_loop(0, tile_dev, live_step, 0, unroll=UNROLL)
    middle = range(regions // 2, regions // 2 + 2)
    for src in range(rim, regions - rim):
        if src not in middle:
            arrived(src)

    @pl.when(jnp.logical_not(down_earlier))
    def _():
        for src in range(1, rim):
            arrived(src)

    pl.when(jnp.logical_and(later[regions - 1], root))(functools.partial(answered, regions - 1))

    def unpack(groups):
        for g in groups:
            for f in range(FIELDS):
                fields[f, group * g : group * (g + 1), :] = landed[g, pl.ds(f, group, stride=FIELDS), :]

    def pair_features(a, b):
        x, y, z, h, m = (fields[f, a:b, :] for f in range(FIELDS))
        norm_sq = x * x + y * y + z * z
        zero, one = jnp.zeros_like(x), jnp.ones_like(x)
        mass_log2 = jnp.where(live[a:b, :] > 0, jnp.log2(m), DEAD_LOG2)
        scale = LOG2E / (h * h)
        own_const = NORM_LOG2 - 3.0 * jnp.log2(h) - scale * norm_sq
        twice = 2.0 * scale
        for k, v in enumerate((x, y, z, norm_sq, one, mass_log2, zero, zero)):
            partner8[pl.ds(8 * a + k, b - a, stride=8), :] = v
        for k, v in enumerate((twice * x, twice * y, twice * z, -scale, own_const, one, zero, zero)):
            own8[pl.ds(8 * a + k, b - a, stride=8), :] = v

        def partner_step(e, carry):
            hi, mid, lo = split3(partner8[pl.ds(pl.multiple_of(e * 8, 8), 8), :])
            partner_t[e] = jnp.concatenate([hi, mid, hi, mid, lo, hi], axis=0).T.astype(BF16)
            return carry

        lax.fori_loop(a, b, partner_step, 0, unroll=largest(b - a))

    def density_of(e, partners, slot):
        hi, mid, lo = split3(own8[pl.ds(pl.multiple_of(e * 8, 8), 8), :])
        mine = jnp.concatenate([hi, hi, mid, mid, hi, lo], axis=0).astype(BF16)
        total = None
        for nb, partner in enumerate(partners):
            w = jnp.exp2(jnp.dot(partner_t[partner], mine, preferred_element_type=F32))
            part = jnp.sum(w.reshape(rows // 8, 8, rows), axis=0)
            total = part if total is None else total + part
            if slot is not None:
                high = w.astype(BF16)
                weight_hi[slot, nb * rows : (nb + 1) * rows, :] = high
                weight_lo[slot, nb * rows : (nb + 1) * rows, :] = (w - high.astype(F32)).astype(BF16)
        raw[pl.ds(e, 1), :] = jnp.sum(total, axis=0, keepdims=True)

    def own_partners(t):
        return [lists[nb, t] + HALO for nb in range(4)]

    def pressures(a, b):
        alive = live[a:b, :] > 0
        total = jnp.where(alive, raw[a:b, :], 1.0)
        return jnp.where(alive, jnp.exp2(jnp.log2(total) * (-1.0 / 3.0)), 0.0)

    def force_features(a, b):
        q = pressures(a, b)
        x, y, z = (fields[f, a:b, :] for f in range(3))
        for k, v in enumerate((jnp.ones_like(q), x, y, z, q, q * x, q * y, q * z)):
            force8[pl.ds(8 * a + k, b - a, stride=8), :] = v

        def step(e, carry):
            v = force8[pl.ds(pl.multiple_of(e * 8, 8), 8), :]
            hi = v.astype(BF16).astype(F32)
            force_f[e] = jnp.concatenate([hi, v - hi], axis=0).astype(BF16)
            return carry

        lax.fori_loop(a, b, step, 0, unroll=largest(b - a))

    def force_of(t):
        feats = jnp.concatenate([force_f[p] for p in own_partners(t)], axis=1)
        got = (jnp.dot(feats, weight_hi[t], preferred_element_type=F32)
               + jnp.dot(feats, weight_lo[t], preferred_element_type=F32))
        sums8[pl.ds(pl.multiple_of(t * 8, 8), 8), :] = got[:8] + got[8:]

    def finish(a, b):
        alive = live[RIM + a : RIM + b, :] > 0
        q = pressures(RIM + a, RIM + b)
        h = fields[3, RIM + a : RIM + b, :]
        density_ref[a:b, :] = jnp.where(alive, raw[RIM + a : RIM + b, :], 0.0)
        plain, pressed = (sums8[pl.ds(8 * a + k, b - a, stride=8), :] for k in (0, 4))
        both = q * plain + pressed
        factor = jnp.where(alive, 2.0 / (h * h), 0.0)
        for k in range(3):
            near, far = (sums8[pl.ds(8 * a + j + k, b - a, stride=8), :] for j in (1, 5))
            accel_ref[k, a:b, :] = factor * (fields[k, RIM + a : RIM + b, :] * both - (q * near + far))

    def inner_density(t, carry):
        density_of(t + RIM, own_partners(t), t)
        return carry

    def inner_force(t, carry):
        force_of(t)
        return carry

    low = group + HALO
    gap = (group * middle[0], group * (middle[-1] + 1))
    unpack([g for g in range(rim + 1, rim + regions) if g - rim not in middle])
    pair_features(RIM + group, RIM + gap[0])
    pair_features(RIM + gap[1], top)

    def density_loop(a, b):
        lax.fori_loop(a, b, inner_density, 0, unroll=largest(b - a))

    density_loop(low, gap[0] - HALO)
    density_loop(gap[1] + HALO, tile_dev - HALO)
    for src in middle:
        arrived(src)
    unpack([rim + g for g in middle])
    pair_features(RIM + gap[0], RIM + gap[1])
    density_loop(gap[0] - HALO, gap[1] + HALO)
    force_features(RIM + low, top)
    lax.fori_loop(low + HALO, tile_dev - RIM, inner_force, 0, unroll=largest(tile_dev - RIM - low - HALO))

    @pl.when(jnp.logical_not(down_earlier))
    def _():
        arrived(0)
        answered_rim(1)


    for copy in metas[0] + metas[1]:
        copy.wait_recv()
    moves = [pltpu.make_async_copy(rim_counts_v, rim_counts, meta_sem.at[0]),
             pltpu.make_async_copy(rim_lists_v, rim_lists, meta_sem.at[1])]
    for move in moves:
        move.start()
    for move in moves:
        move.wait()
    for k in range(RIM):
        live[k : k + 1, :] = (lane < rim_counts[0, 0, tile_dev - RIM + k]).astype(F32)
        live[top + k : top + k + 1, :] = (lane < rim_counts[1, 0, k]).astype(F32)

    rims[1].wait_recv()
    unpack([rim] + list(range(rim + regions, 2 * rim + regions)))
    pair_features(RIM, RIM + group)
    pair_features(top, top + RIM)
    for t in range(HALO, low):
        density_of(RIM + t, own_partners(t), t)
    for k in range(HALO):
        density_of(top - HALO + k, own_partners(tile_dev - HALO + k), tile_dev - HALO + k)
        above = [rim_lists[1, nb, k] + (HALO + tile_dev) for nb in range(4)]
        density_of(top + k, above, None)
    force_features(RIM + HALO, RIM + low)
    force_features(top - RIM, top + RIM)
    for t in list(range(RIM, low + HALO)) + list(range(tile_dev - RIM, tile_dev)):
        force_of(t)
    finish(RIM, tile_dev)

    pl.when(jnp.logical_not(gets_direct))(rims[0].wait_recv)

    @pl.when(gets_direct)
    def _():
        for g in range(rim):
            pltpu.make_async_remote_copy(
                src_ref=packed.at[g], dst_ref=landed.at[g], send_sem=direct_send.at[0],
                recv_sem=direct_recv.at[g], device_id=(r, down), device_id_type=MESH).wait_recv()

    unpack(range(rim))
    pair_features(0, RIM)
    for k in range(HALO):
        below = [jnp.maximum(rim_lists[0, nb, tile_dev - HALO + k] + (HALO - tile_dev), 0) for nb in range(4)]
        density_of(HALO + k, below, None)
        density_of(RIM + k, own_partners(k), k)
    force_features(0, 2 * RIM)
    for k in range(RIM):
        force_of(k)
    finish(0, RIM)
    when_each([mine != k for k in range(regions)], lambda n: copies[n].wait_send())
    pl.when(jnp.logical_not(skips_rim))(rims[0].wait_send)

    @pl.when(gives_direct)
    def _():
        for copy in direct:
            copy.wait_send()

    for copy in metas[0] + metas[1] + rims[1:]:
        copy.wait_send()


def store_kernel(density, accel, density_hbm, accel_hbm, sem):
    copies = [pltpu.make_async_copy(density, density_hbm, sem.at[0]), pltpu.make_async_copy(accel, accel_hbm, sem.at[1])]
    for copy in copies:
        copy.start()
    for copy in copies:
        copy.wait()


def per_device(coords, smooth, masses, owners, counts, neighbours):
    regions, subs = lax.axis_size("region"), lax.axis_size("sub")
    tile_dev, rows = smooth.shape
    group = tile_dev // regions
    rim = RIM // group
    groups = regions + 2 * rim
    ext = tile_dev + 2 * RIM
    owners, counts, lists = owners.reshape(1, -1), counts.reshape(1, -1), neighbours.T
    vmem = pl.BlockSpec(memory_space=pltpu.VMEM)
    dma = pltpu.SemaphoreType.DMA
    density, accel = pl.pallas_call(
        functools.partial(kernel, regions, subs),
        out_shape=(pltpu.VMEM((tile_dev, rows), F32), pltpu.VMEM((3, tile_dev, rows), F32)),
        in_specs=[pl.BlockSpec(memory_space=pl.ANY)] * 6,
        out_specs=(vmem, vmem),
        scratch_shapes=[
            pltpu.VMEM(coords.shape, F32), pltpu.VMEM(smooth.shape, F32), pltpu.VMEM(masses.shape, F32),
            pltpu.VMEM(owners.shape, jnp.int32),
            pltpu.SMEM(counts.shape, jnp.int32), pltpu.SMEM(lists.shape, jnp.int32),
            pltpu.VMEM((2,) + counts.shape, jnp.int32), pltpu.VMEM((2,) + lists.shape, jnp.int32),
            pltpu.SMEM((2,) + counts.shape, jnp.int32), pltpu.SMEM((2,) + lists.shape, jnp.int32),
            pltpu.VMEM((regions, group * FIELDS, rows), F32),
            pltpu.VMEM((groups, group * FIELDS, rows), F32),
            pltpu.VMEM((FIELDS, ext, rows), F32),
            pltpu.VMEM((ext, rows), F32),
            pltpu.VMEM((ext * 8, rows), F32),
            pltpu.VMEM((ext * 8, rows), F32),
            pltpu.VMEM((ext, rows, 48), BF16),
            pltpu.VMEM((tile_dev, 4 * rows, rows), BF16),
            pltpu.VMEM((tile_dev, 4 * rows, rows), BF16),
            pltpu.VMEM((ext, rows), F32),
            pltpu.VMEM((ext * 8, rows), F32),
            pltpu.VMEM((ext, 16, rows), BF16),
            pltpu.VMEM((tile_dev * 8, rows), F32),
            dma((6,)), dma((regions,)), dma((regions,)), dma((2,)), dma((2,)), dma((4,)), dma((4,)), dma((2,)),
            pltpu.SemaphoreType.REGULAR((regions,)), pltpu.SemaphoreType.REGULAR((2,)),
            dma((DIRECT,)), dma((rim,)),
        ],
        compiler_params=pltpu.CompilerParams(collective_id=0, has_side_effects=True),
        name="sph",
    )(coords, smooth, masses, owners, counts, lists)
    return pl.pallas_call(
        store_kernel,
        out_shape=(jax.ShapeDtypeStruct(density.shape, F32), jax.ShapeDtypeStruct(accel.shape, F32)),
        in_specs=[pl.BlockSpec(memory_space=pl.ANY)] * 2,
        out_specs=[pl.BlockSpec(memory_space=pl.ANY)] * 2,
        scratch_shapes=[dma((2,))],
        name="store",
    )(*(pltpu.with_memory_space_constraint(v, pltpu.VMEM) for v in (density, accel)))


def solution(mesh):
    rs = ("region", "sub")
    in_specs = (P(None, rs, None), P(rs, None), P(rs, None), P(rs), P(rs), P(rs, None))
    out_specs = (P(rs, None), P(None, rs, None))
    return jax.shard_map(per_device, mesh=mesh, in_specs=in_specs, out_specs=out_specs, check_vma=False)
```

```python
import functools
import math

import jax
import jax.numpy as jnp
from jax import lax
from jax.experimental import pallas as pl
from jax.experimental.pallas import tpu as pltpu
from jax.sharding import PartitionSpec as P

HALO = 4
RIM = 2 * HALO
FIELDS = 5
UNROLL = 8
DIRECT = 8
SUB_RUN = 12
LOG2E = math.log2(math.e)
NORM_LOG2 = -1.5 * math.log2(math.pi)
DEAD_LOG2 = -1000.0
MESH = pl.DeviceIdType.MESH
F32 = jnp.float32
BF16 = jnp.bfloat16


def largest(n, most=13):
    return max(k for k in range(1, most + 1) if n % k == 0)


def split3(v):
    hi = v.astype(BF16).astype(F32)
    rest = v - hi
    mid = rest.astype(BF16).astype(F32)
    return hi, mid, rest - mid


def kernel(regions, subs, coords_hbm, smooth_hbm, masses_hbm, owners_hbm, counts_hbm, lists_hbm,
           density_ref, accel_ref,
           coords, smooth, masses, owners, counts, lists, rim_counts_v, rim_lists_v, rim_counts, rim_lists,
           packed, landed, fields, live, partner8, own8, partner_t, weight_hi, weight_lo, raw, force8, force_f, sums8,
           in_sem, send_sem, recv_sem, rim_send, rim_recv, meta_send, meta_recv, meta_sem, ok, rim_ok,
           direct_send, direct_recv):
    tile_dev, rows = smooth.shape
    group = tile_dev // regions
    rim = RIM // group
    r = lax.axis_index("region")
    s = lax.axis_index("sub")
    up = lax.rem(s + 1, subs)
    down = lax.rem(s + subs - 1, subs)

    run = lax.rem(s, SUB_RUN) if subs % SUB_RUN == 0 else s
    last_run = (SUB_RUN if subs % SUB_RUN == 0 else subs) - 1
    down_earlier = run > 0
    up_earlier = run == last_run

    def partner(k):
        chips = regions // 2

        def at(k):
            y = k // 2
            return 2 * (y if y < chips // 2 else chips + chips // 2 - 1 - y) + k % 2

        return jnp.where(s == 0, 0 if k == regions - 1 else at(k + 1), at(k))

    def order(i):
        chips = regions // 2
        y = i // 2
        place = 2 * jnp.where(y < chips // 2, y, chips + chips // 2 - 1 - y) + lax.rem(i, 2)
        return jnp.where(s == 0, jnp.where(i == 0, regions - 1, place - 1), place)

    mine = order(r)
    peers = [partner(k) for k in range(regions)]
    later = [mine < k for k in range(regions)]
    earlier = [mine > k for k in range(regions)]

    def when_each(conditions, action):
        for n, condition in enumerate(conditions):
            pl.when(condition)(functools.partial(action, n))

    barrier = pltpu.get_barrier_semaphore()

    def greet(n):
        pl.semaphore_signal(barrier, inc=1, device_id=(peers[n], s), device_id_type=MESH)

    when_each(later, greet)

    def greet_rim(n):
        pl.semaphore_signal(barrier, inc=1, device_id=(r, (up, down)[n]), device_id_type=MESH)

    when_each([jnp.logical_not(up_earlier), jnp.logical_not(down_earlier)], greet_rim)
    ahead = r >= regions - rim
    gets_direct = jnp.logical_and(jnp.logical_not(down_earlier), r < DIRECT)
    skips_rim = jnp.logical_and(up_earlier, r < DIRECT)
    gives_direct = jnp.logical_and(up_earlier, ahead)

    @pl.when(gets_direct)
    def _():
        for g in range(regions - rim, regions):
            pl.semaphore_signal(barrier, inc=1, device_id=(g, down), device_id_type=MESH)

    loads = [pltpu.make_async_copy(src, dst, in_sem.at[n]) for n, (src, dst) in enumerate((
        (owners_hbm, owners), (coords_hbm, coords), (smooth_hbm, smooth), (masses_hbm, masses),
        (counts_hbm, counts), (lists_hbm, lists)))]
    for load in loads:
        load.start()
    expected = mine + down_earlier.astype(jnp.int32) + up_earlier.astype(jnp.int32) + jnp.where(gives_direct, DIRECT, 0)

    @pl.when(expected > 0)
    def _():
        pl.semaphore_wait(barrier, expected)

    def answer(n):
        pl.semaphore_signal(ok.at[r], inc=1, device_id=(peers[n], s), device_id_type=MESH)

    when_each(earlier, answer)

    def answer_rim(n):
        pl.semaphore_signal(rim_ok.at[1 - n], inc=1, device_id=(r, (up, down)[n]), device_id_type=MESH)

    when_each([up_earlier, down_earlier], answer_rim)

    loads[0].wait()
    own = owners[...]
    hot = (lax.broadcasted_iota(jnp.int32, (regions, tile_dev), 0) == own).astype(F32)
    before = (lax.broadcasted_iota(jnp.int32, (tile_dev, tile_dev), 0)
              < lax.broadcasted_iota(jnp.int32, (tile_dev, tile_dev), 1)).astype(F32)
    count = jnp.dot(hot.astype(BF16), before.astype(BF16), preferred_element_type=F32)
    rank = jnp.sum(hot * count, axis=0, keepdims=True).astype(jnp.int32)
    place = own * 8 + rank
    pick = (lax.broadcasted_iota(jnp.int32, (8 * regions, tile_dev), 0) == place).astype(F32)
    pick3 = jnp.concatenate([pick, pick, pick], axis=1).astype(BF16)
    for load in loads[1:4]:
        load.wait()
    for f in range(FIELDS):
        field = coords[f] if f < 3 else (smooth[...] if f == 3 else masses[...])
        stack = jnp.concatenate(split3(field), axis=0).astype(BF16)
        got = jnp.dot(pick3, stack, preferred_element_type=F32)
        for d in range(regions):
            packed[d, pl.ds(f, group, stride=FIELDS), :] = got[8 * d : 8 * d + group]

    copies = [pltpu.make_async_remote_copy(
        src_ref=packed.at[dst], dst_ref=landed.at[rim + r], send_sem=send_sem.at[n],
        recv_sem=recv_sem.at[r], device_id=(dst, s), device_id_type=MESH) for n, dst in enumerate(peers)]
    metas = [[
        pltpu.make_async_remote_copy(
            src_ref=src, dst_ref=dst.at[slot], send_sem=meta_send.at[2 * n + slot],
            recv_sem=meta_recv.at[2 * n + slot], device_id=(r, peer), device_id_type=MESH)
        for n, (src, dst) in enumerate(((counts_hbm, rim_counts_v), (lists_hbm, rim_lists_v)))]
        for slot, peer in enumerate((up, down))]
    rims = [
        pltpu.make_async_remote_copy(
            src_ref=landed.at[pl.ds(regions, rim)], dst_ref=landed.at[pl.ds(0, rim)],
            send_sem=rim_send.at[0], recv_sem=rim_recv.at[0], device_id=(r, up), device_id_type=MESH),
        pltpu.make_async_remote_copy(
            src_ref=landed.at[pl.ds(rim, rim)], dst_ref=landed.at[pl.ds(rim + regions, rim)],
            send_sem=rim_send.at[1], recv_sem=rim_recv.at[1], device_id=(r, down), device_id_type=MESH),
    ]

    def send_meta(slot):
        for copy in metas[slot]:
            copy.start()

    def send_rim(slot):
        rims[slot].start()

    def answered_rim(slot):
        pl.semaphore_wait(rim_ok.at[slot], 1)
        send_meta(slot)
        send_rim(slot)

    def arrived(src):
        @pl.when(src != r)
        def _():
            pltpu.make_async_remote_copy(
                src_ref=packed.at[src], dst_ref=landed.at[rim + src], send_sem=send_sem.at[0],
                recv_sem=recv_sem.at[src], device_id=(src, s), device_id_type=MESH).wait_recv()

    def answered(n):
        pl.semaphore_wait(ok.at[peers[n]], 1)
        copies[n].start()

    def send_up():
        for src in last:
            arrived(src)
        pl.when(jnp.logical_not(skips_rim))(functools.partial(send_rim, 0))

    top = RIM + tile_dev
    last = range(regions - rim, regions)
    def send_earlier(now):
        for n in reversed(range(regions)):
            pl.when(jnp.logical_and(earlier[n], now))(copies[n].start)

    direct = [pltpu.make_async_remote_copy(
        src_ref=packed.at[d], dst_ref=landed.at[r - (regions - rim)], send_sem=direct_send.at[d],
        recv_sem=direct_recv.at[r - (regions - rim)], device_id=(d, up), device_id_type=MESH) for d in range(DIRECT)]

    @pl.when(gives_direct)
    def _():
        for d in [1] + list(range(DIRECT - 1, 1, -1)) + [0]:
            direct[d].start()

    send_earlier(ahead)
    when_each([up_earlier, down_earlier], send_meta)
    landed[rim + r] = packed[r]
    when_each(later[: regions - 2], answered)
    ends = jnp.logical_or(r < 2, r >= regions - 2)
    pl.when(jnp.logical_and(up_earlier, ends))(send_up)
    send_earlier(jnp.logical_not(ahead))
    root = s == 0
    pl.when(later[regions - 2])(functools.partial(answered, regions - 2))
    pl.when(jnp.logical_and(later[regions - 1], jnp.logical_not(root)))(functools.partial(answered, regions - 1))
    pl.when(jnp.logical_and(up_earlier, jnp.logical_not(ends)))(send_up)

    @pl.when(jnp.logical_not(up_earlier))
    def _():
        for src in last:
            arrived(src)
        answered_rim(0)

    @pl.when(down_earlier)
    def _():
        for src in range(rim):
            arrived(src)
        send_rim(1)

    lane = lax.broadcasted_iota(jnp.int32, (1, rows), 1)
    for load in loads[4:]:
        load.wait()

    def live_step(t, carry):
        live[pl.ds(t + RIM, 1), :] = (lane < counts[0, t]).astype(F32)
        return carry

    lax.fori_loop(0, tile_dev, live_step, 0, unroll=UNROLL)
    for src in range(rim, regions - rim):
        arrived(src)

    @pl.when(jnp.logical_not(down_earlier))
    def _():
        for src in range(1, rim):
            arrived(src)

    pl.when(jnp.logical_and(later[regions - 1], root))(functools.partial(answered, regions - 1))

    def unpack(groups):
        for g in groups:
            for f in range(FIELDS):
                fields[f, group * g : group * (g + 1), :] = landed[g, pl.ds(f, group, stride=FIELDS), :]

    def pair_features(a, b):
        x, y, z, h, m = (fields[f, a:b, :] for f in range(FIELDS))
        norm_sq = x * x + y * y + z * z
        zero, one = jnp.zeros_like(x), jnp.ones_like(x)
        mass_log2 = jnp.where(live[a:b, :] > 0, jnp.log2(m), DEAD_LOG2)
        scale = LOG2E / (h * h)
        own_const = NORM_LOG2 - 3.0 * jnp.log2(h) - scale * norm_sq
        twice = 2.0 * scale
        for k, v in enumerate((x, y, z, norm_sq, one, mass_log2, zero, zero)):
            partner8[pl.ds(8 * a + k, b - a, stride=8), :] = v
        for k, v in enumerate((twice * x, twice * y, twice * z, -scale, own_const, one, zero, zero)):
            own8[pl.ds(8 * a + k, b - a, stride=8), :] = v

        def partner_step(e, carry):
            hi, mid, lo = split3(partner8[pl.ds(pl.multiple_of(e * 8, 8), 8), :])
            partner_t[e] = jnp.concatenate([hi, mid, hi, mid, lo, hi], axis=0).T.astype(BF16)
            return carry

        lax.fori_loop(a, b, partner_step, 0, unroll=largest(b - a))

    def density_of(e, partners, slot):
        hi, mid, lo = split3(own8[pl.ds(pl.multiple_of(e * 8, 8), 8), :])
        mine = jnp.concatenate([hi, hi, mid, mid, hi, lo], axis=0).astype(BF16)
        total = None
        for nb, partner in enumerate(partners):
            w = jnp.exp2(jnp.dot(partner_t[partner], mine, preferred_element_type=F32))
            part = jnp.sum(w.reshape(rows // 8, 8, rows), axis=0)
            total = part if total is None else total + part
            if slot is not None:
                high = w.astype(BF16)
                weight_hi[slot, nb * rows : (nb + 1) * rows, :] = high
                weight_lo[slot, nb * rows : (nb + 1) * rows, :] = (w - high.astype(F32)).astype(BF16)
        raw[pl.ds(e, 1), :] = jnp.sum(total, axis=0, keepdims=True)

    def own_partners(t):
        return [lists[nb, t] + HALO for nb in range(4)]

    def pressures(a, b):
        alive = live[a:b, :] > 0
        total = jnp.where(alive, raw[a:b, :], 1.0)
        return jnp.where(alive, jnp.exp2(jnp.log2(total) * (-1.0 / 3.0)), 0.0)

    def force_features(a, b):
        q = pressures(a, b)
        x, y, z = (fields[f, a:b, :] for f in range(3))
        for k, v in enumerate((jnp.ones_like(q), x, y, z, q, q * x, q * y, q * z)):
            force8[pl.ds(8 * a + k, b - a, stride=8), :] = v

        def step(e, carry):
            v = force8[pl.ds(pl.multiple_of(e * 8, 8), 8), :]
            hi = v.astype(BF16).astype(F32)
            force_f[e] = jnp.concatenate([hi, v - hi], axis=0).astype(BF16)
            return carry

        lax.fori_loop(a, b, step, 0, unroll=largest(b - a))

    def force_of(t):
        feats = jnp.concatenate([force_f[p] for p in own_partners(t)], axis=1)
        got = (jnp.dot(feats, weight_hi[t], preferred_element_type=F32)
               + jnp.dot(feats, weight_lo[t], preferred_element_type=F32))
        sums8[pl.ds(pl.multiple_of(t * 8, 8), 8), :] = got[:8] + got[8:]

    def finish(a, b):
        alive = live[RIM + a : RIM + b, :] > 0
        q = pressures(RIM + a, RIM + b)
        h = fields[3, RIM + a : RIM + b, :]
        density_ref[a:b, :] = jnp.where(alive, raw[RIM + a : RIM + b, :], 0.0)
        plain, pressed = (sums8[pl.ds(8 * a + k, b - a, stride=8), :] for k in (0, 4))
        both = q * plain + pressed
        factor = jnp.where(alive, 2.0 / (h * h), 0.0)
        for k in range(3):
            near, far = (sums8[pl.ds(8 * a + j + k, b - a, stride=8), :] for j in (1, 5))
            accel_ref[k, a:b, :] = factor * (fields[k, RIM + a : RIM + b, :] * both - (q * near + far))

    def inner_density(t, carry):
        density_of(t + RIM, own_partners(t), t)
        return carry

    def inner_force(t, carry):
        force_of(t)
        return carry

    unpack(range(rim + 1, rim + regions))
    pair_features(RIM + group, top)
    low = group + HALO
    lax.fori_loop(low, tile_dev - HALO, inner_density, 0, unroll=largest(tile_dev - HALO - low))
    force_features(RIM + low, top)
    lax.fori_loop(low + HALO, tile_dev - RIM, inner_force, 0, unroll=largest(tile_dev - RIM - low - HALO))

    @pl.when(jnp.logical_not(down_earlier))
    def _():
        arrived(0)
        answered_rim(1)


    for copy in metas[0] + metas[1]:
        copy.wait_recv()
    moves = [pltpu.make_async_copy(rim_counts_v, rim_counts, meta_sem.at[0]),
             pltpu.make_async_copy(rim_lists_v, rim_lists, meta_sem.at[1])]
    for move in moves:
        move.start()
    for move in moves:
        move.wait()
    for k in range(RIM):
        live[k : k + 1, :] = (lane < rim_counts[0, 0, tile_dev - RIM + k]).astype(F32)
        live[top + k : top + k + 1, :] = (lane < rim_counts[1, 0, k]).astype(F32)

    rims[1].wait_recv()
    unpack([rim] + list(range(rim + regions, 2 * rim + regions)))
    pair_features(RIM, RIM + group)
    pair_features(top, top + RIM)
    for t in range(HALO, low):
        density_of(RIM + t, own_partners(t), t)
    for k in range(HALO):
        density_of(top - HALO + k, own_partners(tile_dev - HALO + k), tile_dev - HALO + k)
        above = [rim_lists[1, nb, k] + (HALO + tile_dev) for nb in range(4)]
        density_of(top + k, above, None)
    force_features(RIM + HALO, RIM + low)
    force_features(top - RIM, top + RIM)
    for t in list(range(RIM, low + HALO)) + list(range(tile_dev - RIM, tile_dev)):
        force_of(t)
    finish(RIM, tile_dev)

    pl.when(jnp.logical_not(gets_direct))(rims[0].wait_recv)

    @pl.when(gets_direct)
    def _():
        for g in range(rim):
            pltpu.make_async_remote_copy(
                src_ref=packed.at[g], dst_ref=landed.at[g], send_sem=direct_send.at[0],
                recv_sem=direct_recv.at[g], device_id=(r, down), device_id_type=MESH).wait_recv()

    unpack(range(rim))
    pair_features(0, RIM)
    for k in range(HALO):
        below = [jnp.maximum(rim_lists[0, nb, tile_dev - HALO + k] + (HALO - tile_dev), 0) for nb in range(4)]
        density_of(HALO + k, below, None)
        density_of(RIM + k, own_partners(k), k)
    force_features(0, 2 * RIM)
    for k in range(RIM):
        force_of(k)
    finish(0, RIM)
    when_each([mine != k for k in range(regions)], lambda n: copies[n].wait_send())
    pl.when(jnp.logical_not(skips_rim))(rims[0].wait_send)

    @pl.when(gives_direct)
    def _():
        for copy in direct:
            copy.wait_send()

    for copy in metas[0] + metas[1] + rims[1:]:
        copy.wait_send()


def store_kernel(density, accel, density_hbm, accel_hbm, sem):
    copies = [pltpu.make_async_copy(density, density_hbm, sem.at[0]), pltpu.make_async_copy(accel, accel_hbm, sem.at[1])]
    for copy in copies:
        copy.start()
    for copy in copies:
        copy.wait()


def per_device(coords, smooth, masses, owners, counts, neighbours):
    regions, subs = lax.axis_size("region"), lax.axis_size("sub")
    tile_dev, rows = smooth.shape
    group = tile_dev // regions
    rim = RIM // group
    groups = regions + 2 * rim
    ext = tile_dev + 2 * RIM
    owners, counts, lists = owners.reshape(1, -1), counts.reshape(1, -1), neighbours.T
    vmem = pl.BlockSpec(memory_space=pltpu.VMEM)
    dma = pltpu.SemaphoreType.DMA
    density, accel = pl.pallas_call(
        functools.partial(kernel, regions, subs),
        out_shape=(pltpu.VMEM((tile_dev, rows), F32), pltpu.VMEM((3, tile_dev, rows), F32)),
        in_specs=[pl.BlockSpec(memory_space=pl.ANY)] * 6,
        out_specs=(vmem, vmem),
        scratch_shapes=[
            pltpu.VMEM(coords.shape, F32), pltpu.VMEM(smooth.shape, F32), pltpu.VMEM(masses.shape, F32),
            pltpu.VMEM(owners.shape, jnp.int32),
            pltpu.SMEM(counts.shape, jnp.int32), pltpu.SMEM(lists.shape, jnp.int32),
            pltpu.VMEM((2,) + counts.shape, jnp.int32), pltpu.VMEM((2,) + lists.shape, jnp.int32),
            pltpu.SMEM((2,) + counts.shape, jnp.int32), pltpu.SMEM((2,) + lists.shape, jnp.int32),
            pltpu.VMEM((regions, group * FIELDS, rows), F32),
            pltpu.VMEM((groups, group * FIELDS, rows), F32),
            pltpu.VMEM((FIELDS, ext, rows), F32),
            pltpu.VMEM((ext, rows), F32),
            pltpu.VMEM((ext * 8, rows), F32),
            pltpu.VMEM((ext * 8, rows), F32),
            pltpu.VMEM((ext, rows, 48), BF16),
            pltpu.VMEM((tile_dev, 4 * rows, rows), BF16),
            pltpu.VMEM((tile_dev, 4 * rows, rows), BF16),
            pltpu.VMEM((ext, rows), F32),
            pltpu.VMEM((ext * 8, rows), F32),
            pltpu.VMEM((ext, 16, rows), BF16),
            pltpu.VMEM((tile_dev * 8, rows), F32),
            dma((6,)), dma((regions,)), dma((regions,)), dma((2,)), dma((2,)), dma((4,)), dma((4,)), dma((2,)),
            pltpu.SemaphoreType.REGULAR((regions,)), pltpu.SemaphoreType.REGULAR((2,)),
            dma((DIRECT,)), dma((rim,)),
        ],
        compiler_params=pltpu.CompilerParams(collective_id=0, has_side_effects=True),
        name="sph",
    )(coords, smooth, masses, owners, counts, lists)
    return pl.pallas_call(
        store_kernel,
        out_shape=(jax.ShapeDtypeStruct(density.shape, F32), jax.ShapeDtypeStruct(accel.shape, F32)),
        in_specs=[pl.BlockSpec(memory_space=pl.ANY)] * 2,
        out_specs=[pl.BlockSpec(memory_space=pl.ANY)] * 2,
        scratch_shapes=[dma((2,))],
        name="store",
    )(*(pltpu.with_memory_space_constraint(v, pltpu.VMEM) for v in (density, accel)))


def solution(mesh):
    rs = ("region", "sub")
    in_specs = (P(None, rs, None), P(rs, None), P(rs, None), P(rs), P(rs), P(rs, None))
    out_specs = (P(rs, None), P(None, rs, None))
    return jax.shard_map(per_device, mesh=mesh, in_specs=in_specs, out_specs=out_specs, check_vma=False)
```
